256 devices in a mesh: expert: 64 (over y, z, core), token: 4 (over x).
Axes of the slice: x: 4, y: 4, z: 8, core: 2. Of those that a mesh axis runs over, the one named last changes fastest.
Arguments:
- cotangent: bfloat16 [32768, 2048], P(('expert', 'token')), may hold values from -6 to 6
- expert_ids: int32 [32768, 6], P(('expert', 'token')), may hold values from 0 to 63, all different within a row; in each aligned block of 128 rows (0 to 127, 128 to 255, ...) at most 14 rows name the same one
- gate_values: float32 [32768, 6], P(('expert', 'token')), may hold values from 0.05 to 0.45
- hidden_pre: bfloat16 [64, 3584, 768], P('expert', 'token'), may hold values from -8 to 8
- up_weight: bfloat16 [64, 2048, 768], P('expert'), may hold values from -0.125 to 0.125
- down_weight: bfloat16 [64, 2048, 768], P('expert'), may hold values from -0.21875 to 0.21875
Outputs:
- input_grad: bfloat16 [32768, 2048], P(('expert', 'token'))
- down_grad: bfloat16 [64, 2048, 768], P('expert', 'token')
The draws below stay inside these ranges and needn't reach their ends.
Inputs may be any that keep to these rules, and one draw needn't show every extreme that they name: `expert_ids`: each row names 6 different experts. Among the 128 rows of one device no expert is named more than 14 times, and in every draw some expert is named exactly 14 times by the rows of some device.
All inputs are finite; a program needn't handle non-finite values.
Results may differ from the reference program's by a relative error of at most 0.007.
Values may be sent and summed in bfloat16 or wider, within the bound.
A program may use at most 128 MiB of HBM per device.

```python
import math
import jax
import jax.numpy as jnp
import numpy as np
from jax import lax

D = 2048
H = 768
TOP = 6
T_DEV = 128
EXPERTS = 64
CAP = 14
SLOTS = 3584
TOKENS = 32768
N_TOKEN = 4


def steps_of(rng, extent, shards, smallest, largest):
    factor_of = 1.0
    for dim, shards_of in shards:
        steps = jax.random.uniform(jax.random.fold_in(jax.random.fold_in(rng, 6), dim), (shards_of,), jnp.float32, smallest / len(shards), largest / len(shards))
        factor_of = factor_of * jnp.repeat(jnp.exp(steps), extent[dim] // shards_of).reshape((-1,) + (1,) * (len(extent) - 1 - dim))
    return factor_of


def assign_block(rng, own, number, rows, number_of, top, reach, lean):
    ranking = jax.random.permutation(rng, number_of)
    crowded, common = shares(number_of, rows * top, reach, lean, True), shares(number_of, rows * top, reach, lean, False)
    places = jnp.arange(number_of)

    def named(tallies, offset_by):
        used = int((tallies > 0).sum())
        fixed = max(1, used // 4)
        passed = fixed + (places - fixed + offset_by * (used - fixed)) % max(1, number_of - fixed)
        return jnp.zeros((number_of,), jnp.int32).at[ranking[jnp.where(places < fixed, places, passed)]].set(jnp.asarray(tallies, jnp.int32))

    tallies = jnp.where(number % 4 == 0, named(crowded, number // 4), named(common, number - number // 4 - 1))
    mixed = jax.random.permutation(jax.random.fold_in(own, 3), number_of)
    donor, receiver = mixed[0:number_of // 2 * 2:2], mixed[1:number_of // 2 * 2:2]
    margin = jnp.minimum(tallies[donor] - 1, reach - tallies[receiver]) // 2
    margin = jnp.where((donor == ranking[0]) | (receiver == ranking[0]) | (tallies[receiver] == 0), 0, jnp.maximum(margin, 0))
    passed = jax.random.randint(jax.random.fold_in(own, 4), (number_of // 2,), 0, 1 << 20) % (margin + 1)
    tallies = tallies.at[donor].add(-passed).at[receiver].add(passed)
    members = jnp.searchsorted(jnp.cumsum(tallies), jnp.arange(rows * top), side="right").astype(jnp.int32)
    listing = members.reshape(top, rows).T
    listing = listing[jax.random.permutation(jax.random.fold_in(own, 1), rows)]
    offset_by = jax.random.randint(jax.random.fold_in(own, 2), (rows, 1), 0, top)
    return jnp.take_along_axis(listing, (jnp.arange(top)[None, :] + offset_by) % top, axis=1)


def shares(amount, total, bound, lean, full):
    loads = [(1 << 20) // math.isqrt(grade ** lean) + 1 for grade in range(1, amount + 1)]
    largest = bound if full else min(bound, max(-(-total // amount), total * loads[0] // sum(loads)))
    least = 1 if total - largest >= amount - 1 else 0
    holding, rest = [largest] + [least] * (amount - 1), total - largest - least * (amount - 1)
    while rest > 0:
        free = [i for i in range(1, amount) if holding[i] < largest] or [i for i in range(1, amount) if holding[i] < bound]
        pool, budget = sum([loads[i] for i in free]), rest
        for i in free:
            addition = min(bound - holding[i], max(1, budget * loads[i] // pool), rest)
            holding[i] = holding[i] + addition
            rest = rest - addition
    return np.array(holding)


def scatter_about(rng, dims, scale, bound, split=(), kind=jnp.bfloat16):
    factor_of = steps_of(rng, dims, split, -0.22, 0.18) if split else 1.0
    values = jax.random.normal(rng, dims, jnp.float32) * scale * factor_of
    return jnp.minimum(jnp.maximum(values, -bound), bound).astype(kind)


def setup_inputs(seed: int = 0) -> dict:
    splits = jax.random.split(jax.random.key(seed), 7)
    cotangent = scatter_about(splits[0], (TOKENS, D), 1.0, 6.0, ((0, 256),))
    expert_ids_keys = jax.random.split(jax.random.fold_in(splits[1], 1), TOKENS // T_DEV)
    expert_ids_turns = jax.random.permutation(jax.random.fold_in(splits[1], 3), TOKENS // T_DEV)
    expert_ids = jax.vmap(lambda own, number: assign_block(jax.random.fold_in(splits[1], 2), own, number, T_DEV, EXPERTS, TOP, CAP, 2))(expert_ids_keys, expert_ids_turns).reshape((TOKENS, TOP))
    gate_values = jnp.clip(0.05 + 0.39999999 * jax.random.uniform(splits[2], (TOKENS, TOP), jnp.float32) ** steps_of(splits[2], (TOKENS, TOP), ((0, 256),), -0.2, 0.2), 0.05, 0.45)
    hidden_pre = scatter_about(splits[3], (EXPERTS, SLOTS, H), 1.5, 8.0, ((0, 64), (1, 4)))
    up_weight = scatter_about(splits[4], (EXPERTS, D, H), D ** -0.5, 0.125, ((0, 64),))
    down_weight = scatter_about(splits[5], (EXPERTS, D, H), H ** -0.5, 0.21875, ((0, 64),))
    return {"cotangent": cotangent, "expert_ids": expert_ids, "gate_values": gate_values, "hidden_pre": hidden_pre, "up_weight": up_weight, "down_weight": down_weight}


grad_scale = 0.03125
root_half = 0.7071067811865476
inv_root_two_pi = 0.3989422804014327


def slope_and_act(hidden_rows):
    values = hidden_rows.astype(jnp.float32)
    normal_cdf = 0.5 * (1.0 + lax.erf(values * root_half))
    density = inv_root_two_pi * jnp.exp(-0.5 * values * values)
    slopes = normal_cdf + values * density
    active = (values * normal_cdf).astype(jnp.bfloat16)
    return slopes, active


def slot_tables(expert_ids, gate_values, slot_count):
    top_count = expert_ids.shape[1]
    blocks = expert_ids.shape[0] // T_DEV
    grouped = expert_ids.reshape(blocks, T_DEV * top_count)
    one_hot = (grouped[:, :, None] == jnp.arange(EXPERTS, dtype=jnp.int32)[None, None, :]).astype(jnp.int32)
    earlier = jnp.cumsum(one_hot, axis=1) - one_hot
    rank_in = jnp.sum(earlier * one_hot, axis=2).astype(jnp.int32)
    block_ids = jnp.arange(blocks, dtype=jnp.int32)[:, None]
    slot_row = (block_ids % N_TOKEN) * (EXPERTS * CAP) + (block_ids // N_TOKEN) * CAP + rank_in
    token_ids = block_ids * T_DEV + jnp.arange(T_DEV * top_count, dtype=jnp.int32)[None, :] // top_count
    flat_expert = grouped.reshape(-1).astype(jnp.int32)
    flat_slot = slot_row.reshape(-1).astype(jnp.int32)
    slot_token = jnp.zeros((EXPERTS, slot_count), jnp.int32).at[flat_expert, flat_slot].set(token_ids.reshape(-1).astype(jnp.int32))
    slot_gate = jnp.zeros((EXPERTS, slot_count), jnp.float32).at[flat_expert, flat_slot].set(gate_values.reshape(-1))
    slot_live = jnp.zeros((EXPERTS, slot_count), jnp.float32).at[flat_expert, flat_slot].set(jnp.ones_like(gate_values.reshape(-1)))
    return slot_token, slot_gate, slot_live


def apply_transpose(token_rows, slot_token, slot_gate, slot_live, hidden_pre, up_weight, down_weight):
    def per_expert(summed, stacked):
        token_ids, gate_e, live_e, hidden_e, up_e, down_e = stacked
        slopes, unused_act = slope_and_act(hidden_e)
        gathered = jnp.take(token_rows, token_ids, axis=0)
        gathered = jnp.where(live_e[:, None] > 0.5, gathered, jnp.zeros_like(gathered))
        inner_prod = jnp.dot(gathered, down_e, preferred_element_type=jnp.float32)
        scaled = (inner_prod * slopes).astype(jnp.bfloat16)
        pieces = jnp.dot(scaled, up_e.T, preferred_element_type=jnp.float32).astype(jnp.bfloat16)
        weighted = pieces.astype(jnp.float32) * gate_e[:, None]
        summed = summed.at[token_ids].add(weighted)
        return summed, jnp.zeros((), jnp.float32)

    initial = jnp.zeros(token_rows.shape, jnp.float32)
    summed, unused_out = lax.scan(per_expert, initial, (slot_token, slot_gate, slot_live, hidden_pre, up_weight, down_weight))
    return summed.astype(jnp.bfloat16)


def reference(cotangent, expert_ids, gate_values, hidden_pre, up_weight, down_weight):
    slot_token, slot_gate, slot_live = slot_tables(expert_ids, gate_values, hidden_pre.shape[1])
    first_term = apply_transpose(cotangent, slot_token, slot_gate, slot_live, hidden_pre, up_weight, down_weight)
    second = apply_transpose(first_term, slot_token, slot_gate, slot_live, hidden_pre, up_weight, down_weight)
    input_grad = (cotangent.astype(jnp.float32) + first_term.astype(jnp.float32) + second.astype(jnp.float32)).astype(jnp.bfloat16)

    def grad_expert(carried, stacked):
        token_ids, gate_e, hidden_e = stacked
        unused_slope, active = slope_and_act(hidden_e)
        picked = jnp.take(input_grad, token_ids, axis=0).astype(jnp.float32)
        routed = (picked * gate_e[:, None]).astype(jnp.bfloat16)
        grad_e = jnp.dot(routed.T, active, preferred_element_type=jnp.float32)
        return carried, (grad_e * grad_scale).astype(jnp.bfloat16)

    unused_carry, down_grad = lax.scan(grad_expert, jnp.zeros((), jnp.float32), (slot_token, slot_gate, hidden_pre))
    return input_grad, down_grad
```

```python
import jax
import jax.numpy as jnp
from jax import lax
from jax.experimental import pallas as pl
from jax.experimental.pallas import tpu as pltpu
from jax.sharding import PartitionSpec as P

grad_scale = 0.03125
root_half = 0.7071067811865476
inv_root_two_pi = 0.3989422804014327

NY, NZ, NC, NX = 4, 8, 2, 4
T = 128
D = 2048
HID = 768
CAP = 14
RB = NZ * CAP
NE = NY * NC
SL = NE * RB
H = 2
NCH = NX * H
W = D // NCH
ZR = NZ * T
NPF = 5
BF = jnp.bfloat16
F32 = jnp.float32
MESH = pl.DeviceIdType.MESH


def slope_and_act(hidden_rows):
    values = hidden_rows.astype(jnp.float32)
    normal_cdf = 0.5 * (1.0 + lax.erf(values * root_half))
    density = inv_root_two_pi * jnp.exp(-0.5 * values * values)
    slopes = normal_cdf + values * density
    active = (values * normal_cdf).astype(jnp.bfloat16)
    return (slopes, active)


def kernel(
    cot_hbm, tg_hbm, slope_hbm, act_hbm, up_hbm, down_hbm,
    ig_ref, dg_ref,
    CV, TV, TGR, SV, AX, UV, DV, PM, PT, G, ZB, YS, RL, RV, QL, QV, IA, SC, PF, RSS, RSR, XS, XR,
    l_zb, l_in, tg_s, tg_r, ax_s, ax_r,
    z_s, z_r, y_s, rl_r, f_s, rv_r, ql_r, qv_r, rs_s, rs_r, x_s, x_r,
):
    ex = lax.axis_index("expert")
    x = lax.axis_index("token")
    y = ex // (NZ * NC)
    z = (ex // NC) % NZ
    c = ex % NC
    me = y * NC + c
    yp, ym, y2 = (y + 1) % NY, (y + NY - 1) % NY, (y + 2) % NY

    def dev(yy, zz, cc, xx):
        return ((yy * NZ + zz) * NC + cc, xx)

    def remote(src, dst, ssem, rsem, target):
        return pltpu.make_async_remote_copy(
            src_ref=src, dst_ref=dst, send_sem=ssem, recv_sem=rsem, device_id=target, device_id_type=MESH
        )

    partner = dev(y, z, 1 - c, x)

    def wait_recv(ref, rsem):
        remote(ref, ref, tg_s.at[0], rsem, partner).wait_recv()

    def wait_send(ref, ssem):
        remote(ref, ref, ssem, tg_r.at[0], partner).wait_send()

    def col(i):
        return (i + x * H) % NCH

    def zrow(b):
        return pl.ds(pl.multiple_of(b * T, T), T)

    zme = zrow(z)

    def zb_in(i):
        return pltpu.make_async_copy(cot_hbm.at[col(i)], ZB.at[i, zme, :], l_zb.at[i])

    ins = [
        pltpu.make_async_copy(tg_hbm, TV, l_in.at[0]),
        pltpu.make_async_copy(down_hbm, DV, l_in.at[1]),
        pltpu.make_async_copy(slope_hbm, SV, l_in.at[2]),
        pltpu.make_async_copy(up_hbm, UV, l_in.at[3]),
        pltpu.make_async_copy(cot_hbm, CV, l_in.at[4]),
        pltpu.make_async_copy(act_hbm, AX.at[x], l_in.at[5]),
    ]
    ins[0].start()

    @pl.loop(0, NCH)
    def _(i):
        zb_in(i).start()

    for copy in ins[1:]:
        copy.start()
    ins[0].wait()

    @pl.loop(1, NX * NZ)
    def _(q):
        xx = (x + q // NZ) % NX
        zz = (z + q) % NZ
        remote(TV.at[zz], TGR.at[x, z], tg_s.at[0], tg_r.at[x], dev(y, zz, c, xx)).start()

    TGR[x, z] = TV[z]
    for dx in range(1, NX):
        remote(act_hbm, AX.at[x], ax_s.at[0], ax_r.at[x], dev(y, z, c, (x + dx) % NX)).start()

    @pl.loop(0, NCH)
    def _(i):
        for o in range(NE):
            QV[i, o * T + RB : (o + 1) * T, :] = jnp.zeros((T - RB, W), BF)

    def build(xs, with_pt):
        @pl.loop(0, NE)
        def _(o):
            gsum = jnp.zeros((RB, 1), F32)
            rows = pl.ds(pl.multiple_of(o * RB, 16), RB)
            for s in range(NZ):
                rank = TGR[xs, s, pl.ds(o, 1), :]
                gate = TGR[xs, s, pl.ds(NE + o, 1), :]
                slot = jnp.where(rank >= 0.0, rank + float(s * CAP), -1.0)
                iota = lax.broadcasted_iota(jnp.int32, (T, T), 0).astype(F32)
                hit = jnp.where(iota == slot, 1.0, 0.0)
                PM[rows, s * T : (s + 1) * T] = hit[:RB].astype(BF)
                gsum = gsum + jnp.sum(hit[:RB] * gate, axis=1, keepdims=True)
                if with_pt:
                    PT[s * T : (s + 1) * T, pl.ds(pl.multiple_of(o * T, T), T)] = hit.T.astype(BF)
            G[rows, :] = jnp.broadcast_to(gsum, (RB, 128))

    def y_send(i, dst, pitch, rsem, relay, relay_r):
        mine = dst.at[i, pl.ds(pl.multiple_of(me * pitch, 16), RB), :]

        def src(yy, cc):
            return YS.at[i, pl.ds(pl.multiple_of((yy * NC + cc) * RB, 16), RB), :]

        remote(src(y2, 0), relay.at[i, 0], y_s.at[i], relay_r.at[0, i], dev(yp, z, c, x)).start()
        remote(src(y2, 1), relay.at[i, 1], y_s.at[i], relay_r.at[1, i], dev(ym, z, c, x)).start()
        for cc in range(NC):
            remote(src(yp, cc), mine, y_s.at[i], rsem.at[me, i], dev(yp, z, cc, x)).start()
            remote(src(ym, cc), mine, y_s.at[i], rsem.at[me, i], dev(ym, z, cc, x)).start()
        remote(src(y, 1 - c), mine, y_s.at[i], rsem.at[me, i], partner).start()
        dst[i, pl.ds(pl.multiple_of(me * pitch, 16), RB), :] = YS[
            i, pl.ds(pl.multiple_of(me * RB, 16), RB), :
        ]

    def y_relay(i, dst, pitch, rsem, relay, relay_r):
        for d, (frm, to) in enumerate(((ym, yp), (yp, ym))):
            o = frm * NC + c
            wait_recv(relay.at[i, d], relay_r.at[d, i])
            remote(
                relay.at[i, d],
                dst.at[i, pl.ds(pl.multiple_of(o * pitch, 16), RB), :],
                f_s.at[i],
                rsem.at[o, i],
                dev(to, z, d, x),
            ).start()

    def y_wait(i, dst, pitch, rsem):
        for q in range(1, NE):
            o = (me + q) % NE
            wait_recv(dst.at[i, pl.ds(pl.multiple_of(o * pitch, 16), RB), :], rsem.at[o, i])

    def y_drain(relay):
        @pl.loop(0, NCH)
        def _(i):
            wait_send(YS.at[i, pl.ds(0, (NE - 1) * RB), :], y_s.at[i])
            wait_send(relay.at[i], f_s.at[i])

    SG = (1, -1)

    def lanes(k, d):
        return pl.ds(d * (W // 2), W // 2) if k == 4 else pl.ds(0, W)

    def z_send(i, k, d, src=None):
        b = (z + NZ - SG[d] * (k - 1)) % NZ
        ref = ZB.at[i, zrow(b), lanes(k, d)]
        remote(
            ref if src is None else src, ref, z_s.at[i], z_r.at[d, k - 1, i], dev(y, (z + NZ + SG[d]) % NZ, c, x)
        ).start()

    def z_wait(i, k, d):
        b = (z + NZ - SG[d] * k) % NZ
        wait_recv(ZB.at[i, zrow(b), lanes(k, d)], z_r.at[d, k - 1, i])

    def r_lanes(k, d):
        return pl.ds(d * (W // 2), W // 2) if k == 1 else pl.ds(0, W)

    def r_send(i, k, d):
        ln = r_lanes(k, d)
        remote(
            RSS.at[i, d, k - 1, :, ln],
            RSR.at[i, d, k - 1, :, ln],
            rs_s.at[i],
            rs_r.at[d, k - 1, i],
            dev(y, (z + NZ + SG[d]) % NZ, c, x),
        ).start()

    def r_wait(i, k, d):
        wait_recv(RSR.at[i, d, k - 1, :, r_lanes(k, d)], rs_r.at[d, k - 1, i])

    def when_chunk(t, lag):
        i = t - lag
        return i, pl.when((i >= 0) & (i < NCH))

    def dispatch(p, consume, last):
        @pl.loop(0, NCH + 6)
        def _(t):
            for k in (4, 3, 2):
                i, guard = when_chunk(t, k - 1)

                @guard
                def _(i=i, k=k):
                    for d in range(2):
                        z_wait(i, k - 1, d)
                        z_send(i, k, d)

            i, guard = when_chunk(t, 0)

            @guard
            def _(i=i):
                if last:
                    @pl.when(i >= H)
                    def _():
                        wait_recv(XR.at[i], x_r.at[i])

                    for d in range(2):
                        z_send(i, 1, d, XR.at[i])
                    ZB[i, zme, :] = XR[i]
                else:
                    @pl.when(p == 0)
                    def _():
                        zb_in(i).wait()

                    for d in range(2):
                        z_send(i, 1, d)

            if not last:
                @pl.when((p == 0) & (t == 2))
                def _():
                    wait_recv(TGR.at[x, pl.ds(0, NZ - 1)], tg_r.at[x])
                    for dx in range(1, NX):
                        xs = (x + dx) % NX
                        wait_recv(TGR.at[xs], tg_r.at[xs])
                    build(x, True)
                    for copy in ins[1:]:
                        copy.wait()

            i, guard = when_chunk(t, 5)

            @guard
            def _(i=i):
                y_relay(i, RV, RB, rv_r, RL, rl_r)

            i, guard = when_chunk(t, 4)

            @guard
            def _(i=i):
                for d in range(2):
                    z_wait(i, 4, d)
                if last:
                    @pl.when(i % H == 0)
                    def _():
                        build((x + NX - i // H) % NX, False)

                rows = jnp.dot(PM[...], ZB[i], preferred_element_type=F32)
                for n in range(W // 128):
                    YS[i, :, n * 128 : (n + 1) * 128] = (rows[:, n * 128 : (n + 1) * 128] * G[...]).astype(BF)
                y_send(i, RV, RB, rv_r, RL, rl_r)

            i, guard = when_chunk(t, 6)

            @guard
            def _(i=i):
                y_wait(i, RV, RB, rv_r)
                consume(i)

        @pl.loop(0, NCH)
        def _(i):
            wait_send(ZB.at[i, pl.ds(0, (NZ - 1) * T), :], z_s.at[i])

        y_drain(RL)

    def consume_inner(i):
        rows = pl.ds(pl.multiple_of(col(i) * W, W), W)

        @pl.loop(0, HID // 256)
        def _(n):
            ln = pl.ds(pl.multiple_of(n * 256, 256), 256)
            IA[:, ln] += jnp.dot(RV[i], DV[rows, ln], preferred_element_type=F32)

    def consume_grad(i):
        xs = (x + NX - i // H) % NX

        @pl.when((i % H == 0) & (i > 0))
        def _():
            wait_recv(AX.at[xs], ax_r.at[xs])

        rows = pl.ds(pl.multiple_of((i % H) * W, W), W)
        IA[rows, :] += lax.dot_general(RV[i], AX[xs], (((0,), (0,)), ((), ())), preferred_element_type=F32)

    def give_back(p):
        @pl.loop(0, NCH + 6)
        def _(t):
            i, guard = when_chunk(t, 6)

            @guard
            def _(i=i):
                for d in range(2):
                    r_wait(i, 4, d)
                total = PF[i % NPF, zme, :] + RSR[i, 0, 3].astype(F32) + RSR[i, 1, 3].astype(F32)
                term = total.astype(BF)

                @pl.when(p == 0)
                def _():
                    ZB[i, zme, :] = term

                @pl.when(p == 1)
                def _():
                    j = col(i)
                    grad = (CV[j].astype(F32) + ZB[i, zme, :].astype(F32) + term.astype(F32)).astype(BF)
                    ig_ref[:, pl.ds(pl.multiple_of(j * W, W), W)] = grad

                    @pl.when(i < H)
                    def _():
                        XR[i] = grad

                    @pl.when(i >= H)
                    def _():
                        XS[i] = grad
                        remote(
                            XS.at[i], XR.at[i], x_s.at[i], x_r.at[i], dev(y, z, c, (x + i // H) % NX)
                        ).start()

            for k in (4, 3, 2):
                i, guard = when_chunk(t, k + 1)

                @guard
                def _(i=i, k=k):
                    for d in range(2):
                        r_wait(i, k - 1, d)
                        mine = PF.at[i % NPF, zrow((z + NZ + SG[d] * (5 - k)) % NZ), :]
                        if k == 2:
                            half, rest = pl.ds(d * (W // 2), W // 2), pl.ds((1 - d) * (W // 2), W // 2)
                            RSS[i, d, 1, :, rest] = mine[:, rest].astype(BF)
                            RSS[i, d, 1, :, half] = (mine[:, half] + RSR[i, d, 0, :, half].astype(F32)).astype(BF)
                        else:
                            RSS[i, d, k - 1] = (mine[...] + RSR[i, d, k - 2].astype(F32)).astype(BF)
                        r_send(i, k, d)

            i, guard = when_chunk(t, 1)

            @guard
            def _(i=i):
                y_relay(i, QV, T, qv_r, QL, ql_r)

            i, guard = when_chunk(t, 2)

            @guard
            def _(i=i):
                y_wait(i, QV, T, qv_r)
                PF[i % NPF] = jnp.dot(PT[...], QV[i], preferred_element_type=F32)
                for d in range(2):
                    ln = pl.ds(d * (W // 2), W // 2)
                    RSS[i, d, 0, :, ln] = PF[i % NPF, zrow((z + 4) % NZ), ln].astype(BF)
                    r_send(i, 1, d)

            i, guard = when_chunk(t, 0)

            @guard
            def _(i=i):
                rows = pl.ds(pl.multiple_of(col(i) * W, W), W)
                YS[i] = lax.dot_general(
                    SC[...], UV[rows, :], (((1,), (1,)), ((), ())), preferred_element_type=F32
                ).astype(BF)
                y_send(i, QV, T, qv_r, QL, ql_r)

        @pl.loop(0, NCH)
        def _(i):
            wait_send(ZB.at[i, pl.ds(0, (NZ - 1) * T), :], rs_s.at[i])

        y_drain(QL)

    @pl.loop(0, 2)
    def _(p):
        IA[...] = jnp.zeros_like(IA)
        dispatch(p, consume_inner, False)

        @pl.loop(0, SL // 128)
        def _(n):
            rows = pl.ds(pl.multiple_of(n * 128, 128), 128)
            SC[rows, :] = (IA[rows, :] * SV[rows, :]).astype(BF)

        give_back(p)

    IA[: H * W, :] = jnp.zeros((H * W, HID), F32)
    dispatch(2, consume_grad, True)
    dg_ref[...] = (IA[: H * W, :] * grad_scale).astype(BF)

    @pl.loop(H, NCH)
    def _(i):
        wait_send(XS.at[i], x_s.at[i])

    for _ in range(NX - 1):
        wait_send(AX.at[x], ax_s.at[0])
    wait_send(TGR.at[pl.ds(0, NX - 1)], tg_s.at[0])
    wait_send(TGR.at[x, pl.ds(0, NZ - 1)], tg_s.at[0])


def body(cotangent, expert_ids, gate_values, hidden_pre, up_weight, down_weight):
    experts = NY * NZ * NC
    hidden = hidden_pre[0].reshape(NY, NZ, NC, CAP, HID).transpose(0, 2, 1, 3, 4).reshape(SL, HID)
    slopes, active = slope_and_act(hidden)
    onehot = expert_ids[:, :, None] == jnp.arange(experts, dtype=jnp.int32)[None, None, :]
    named = jnp.any(onehot, axis=1)
    count = named.astype(jnp.int32)
    rank = jnp.cumsum(count, axis=0) - count
    rank = jnp.where(named, rank, -1).astype(F32)
    gate = jnp.sum(jnp.where(onehot, gate_values[:, :, None], 0.0), axis=1)

    def planes(table):
        return table.T.reshape(NY, NZ, NC, T).transpose(1, 0, 2, 3).reshape(NZ, NE, T)

    tables = jnp.concatenate([planes(rank), planes(gate)], axis=1)
    cot = cotangent.reshape(T, NCH, W).transpose(1, 0, 2)

    vm, dma = pltpu.VMEM, pltpu.SemaphoreType.DMA
    input_grad, down_grad = pl.pallas_call(
        kernel,
        out_shape=(jax.ShapeDtypeStruct((T, D), BF), jax.ShapeDtypeStruct((H * W, HID), BF)),
        in_specs=[pl.BlockSpec(memory_space=pl.ANY)] * 6,
        out_specs=(pl.BlockSpec(memory_space=pltpu.VMEM),) * 2,
        scratch_shapes=[
            vm((NCH, T, W), BF),
            vm((NZ, 2 * NE, T), F32),
            vm((NX, NZ, 2 * NE, T), F32),
            vm((SL, HID), F32),
            vm((NX, SL, HID), BF),
            vm((D, HID), BF),
            vm((D, HID), BF),
            vm((SL, ZR), BF),
            vm((ZR, NE * T), BF),
            vm((SL, 128), F32),
            vm((NCH, ZR, W), BF),
            vm((NCH, SL, W), BF),
            vm((NCH, 2, RB, W), BF),
            vm((NCH, SL, W), BF),
            vm((NCH, 2, RB, W), BF),
            vm((NCH, NE * T, W), BF),
            vm((SL, HID), F32),
            vm((SL, HID), BF),
            vm((NPF, ZR, W), F32),
            vm((NCH, 2, 4, T, W), BF),
            vm((NCH, 2, 4, T, W), BF),
            vm((NCH, T, W), BF),
            vm((NCH, T, W), BF),
            dma((NCH,)), dma((6,)), dma((1,)), dma((NX,)), dma((1,)), dma((NX,)),
            dma((NCH,)), dma((2, 4, NCH)), dma((NCH,)), dma((2, NCH)), dma((NCH,)), dma((NE, NCH)),
            dma((2, NCH)), dma((NE, NCH)), dma((NCH,)), dma((2, 4, NCH)), dma((NCH,)), dma((NCH,)),
        ],
        compiler_params=pltpu.CompilerParams(has_side_effects=True, vmem_limit_bytes=67043328),
        name="layer",
    )(cot, tables, slopes, active, up_weight[0], down_weight[0])
    return (input_grad, down_grad[None])


def solution(mesh):
    in_specs = (
        P(("expert", "token"), None),
        P(("expert", "token"), None),
        P(("expert", "token"), None),
        P("expert", "token", None),
        P("expert", None, None),
        P("expert", None, None),
    )
    out_specs = (P(("expert", "token"), None), P("expert", "token", None))
    return jax.shard_map(body, mesh=mesh, in_specs=in_specs, out_specs=out_specs, check_vma=False)
```

```python
import jax
import jax.numpy as jnp
from jax import lax
from jax.experimental import pallas as pl
from jax.experimental.pallas import tpu as pltpu
from jax.sharding import PartitionSpec as P

grad_scale = 0.03125
root_half = 0.7071067811865476
inv_root_two_pi = 0.3989422804014327

NY, NZ, NC, NX = 4, 8, 2, 4
T = 128
D = 2048
HID = 768
CAP = 14
RB = NZ * CAP
NE = NY * NC
SL = NE * RB
H = 2
NCH = NX * H
W = D // NCH
ZR = NZ * T
NPF = 5
BF = jnp.bfloat16
F32 = jnp.float32
MESH = pl.DeviceIdType.MESH


def slope_and_act(hidden_rows):
    values = hidden_rows
    normal_cdf = 0.5 * (1.0 + lax.erf(values * root_half))
    density = inv_root_two_pi * jnp.exp(-0.5 * values * values)
    slopes = normal_cdf + values * density
    active = (values * normal_cdf).astype(jnp.bfloat16)
    return (slopes, active)


def kernel(
    cot_hbm, tg_hbm, hid_hbm, up_hbm, down_hbm,
    ig_ref, dg_ref,
    CV, TV, TGR, HV, SV, AX, UV, DV, PM, PT, G, ZB, YS, RL, RV, QL, QV, IA, SC, PF, RSS, RSR, XS, XR,
    l_zb, l_in, tg_s, tg_r, ax_s, ax_r,
    z_s, z_r, y_s, rl_r, f_s, g_s, rv_r, ql_r, qv_r, rs_s, rs_r, x_s, x_r,
):
    ex = lax.axis_index("expert")
    x = lax.axis_index("token")
    y = ex // (NZ * NC)
    z = (ex // NC) % NZ
    c = ex % NC
    me = y * NC + c
    yp, ym, y2 = (y + 1) % NY, (y + NY - 1) % NY, (y + 2) % NY

    def dev(yy, zz, cc, xx):
        return ((yy * NZ + zz) * NC + cc, xx)

    def remote(src, dst, ssem, rsem, target):
        return pltpu.make_async_remote_copy(
            src_ref=src, dst_ref=dst, send_sem=ssem, recv_sem=rsem, device_id=target, device_id_type=MESH
        )

    partner = dev(y, z, 1 - c, x)

    def wait_recv(ref, rsem):
        remote(ref, ref, tg_s.at[0], rsem, partner).wait_recv()

    def wait_send(ref, ssem):
        remote(ref, ref, ssem, tg_r.at[0], partner).wait_send()

    def col(i):
        return (i + x * H) % NCH

    def wide(j):
        return pl.ds(pl.multiple_of(j * W, W), W)

    def zrow(b):
        return pl.ds(pl.multiple_of(b * T, T), T)

    zme = zrow(z)

    def zb_in(i):
        return pltpu.make_async_copy(cot_hbm.at[:, wide(col(i))], ZB.at[i, zme, :], l_zb.at[i])

    ins = [
        pltpu.make_async_copy(tg_hbm, TV, l_in.at[0]),
        pltpu.make_async_copy(hid_hbm, HV, l_in.at[1]),
        pltpu.make_async_copy(down_hbm, DV, l_in.at[2]),
        pltpu.make_async_copy(up_hbm, UV, l_in.at[3]),
        pltpu.make_async_copy(cot_hbm, CV, l_in.at[4]),
    ]
    ins[0].start()

    @pl.loop(0, NCH)
    def _(i):
        zb_in(i).start()

    for copy in ins[1:]:
        copy.start()
    ins[0].wait()

    @pl.loop(1, NX * NZ)
    def _(q):
        xx = (x + q // NZ) % NX
        zz = (z + q) % NZ
        remote(TV.at[zz], TGR.at[x, z], tg_s.at[0], tg_r.at[x], dev(y, zz, c, xx)).start()

    TGR[x, z] = TV[z]
    @pl.loop(0, NCH)
    def _(i):
        for o in range(NE):
            QV[i, o * T + RB : (o + 1) * T, :] = jnp.zeros((T - RB, W), BF)

    YB = NZ * NC * CAP

    def activate(b):
        new = lax.broadcasted_iota(jnp.int32, (YB, YB), 0).astype(F32)
        core = jnp.where(new >= float(RB), 1.0, 0.0)
        new = new - core * RB
        plane = jnp.floor((new + 0.5) * (1.0 / CAP))
        old = plane * (NC * CAP) + core * CAP + (new - plane * CAP)
        here = lax.broadcasted_iota(jnp.int32, (YB, YB), 1).astype(F32)
        order = jnp.where(here == old, 1.0, 0.0).astype(BF)
        rows = pl.ds(b * YB, YB)
        hidden = jnp.dot(order, HV[rows, :], preferred_element_type=F32)
        slopes, active = slope_and_act(hidden)
        SV[rows, :] = slopes
        AX[x, rows, :] = active

    def build(xs, with_pt):
        @pl.loop(0, NE)
        def _(o):
            gsum = jnp.zeros((RB, 1), F32)
            rows = pl.ds(pl.multiple_of(o * RB, 16), RB)
            for s in range(NZ):
                rank = TGR[xs, s, pl.ds(o, 1), :]
                gate = TGR[xs, s, pl.ds(NE + o, 1), :]
                slot = jnp.where(rank >= 0.0, rank + float(s * CAP), -1.0)
                iota = lax.broadcasted_iota(jnp.int32, (T, T), 0).astype(F32)
                hit = jnp.where(iota == slot, 1.0, 0.0)
                PM[rows, s * T : (s + 1) * T] = hit[:RB].astype(BF)
                gsum = gsum + jnp.sum(hit[:RB] * gate, axis=1, keepdims=True)
                if with_pt:
                    PT[s * T : (s + 1) * T, pl.ds(pl.multiple_of(o * T, T), T)] = hit.T.astype(BF)
            G[rows, :] = jnp.broadcast_to(gsum, (RB, 128))

    def y_send(i, dst, pitch, rsem, relay, relay_r):
        mine = dst.at[i, pl.ds(pl.multiple_of(me * pitch, 16), RB), :]

        def src(yy, cc):
            return YS.at[i, pl.ds(pl.multiple_of((yy * NC + cc) * RB, 16), RB), :]

        remote(src(y2, 0), relay.at[i, 0], y_s.at[i], relay_r.at[0, i], dev(yp, z, c, x)).start()
        remote(src(y2, 1), relay.at[i, 1], y_s.at[i], relay_r.at[1, i], dev(ym, z, c, x)).start()
        for cc in range(NC):
            remote(src(yp, cc), mine, y_s.at[i], rsem.at[me, i], dev(yp, z, cc, x)).start()
            remote(src(ym, cc), mine, y_s.at[i], rsem.at[me, i], dev(ym, z, cc, x)).start()
        remote(src(y, 1 - c), mine, y_s.at[i], rsem.at[me, i], partner).start()
        dst[i, pl.ds(pl.multiple_of(me * pitch, 16), RB), :] = YS[
            i, pl.ds(pl.multiple_of(me * RB, 16), RB), :
        ]

    def y_relay(i, dst, pitch, rsem, relay, relay_r, fsem):
        for d, (frm, to) in enumerate(((ym, yp), (yp, ym))):
            o = frm * NC + c
            wait_recv(relay.at[i, d], relay_r.at[d, i])
            remote(
                relay.at[i, d],
                dst.at[i, pl.ds(pl.multiple_of(o * pitch, 16), RB), :],
                fsem.at[i],
                rsem.at[o, i],
                dev(to, z, d, x),
            ).start()

    def y_wait(i, dst, pitch, rsem):
        for q in range(1, NE):
            o = (me + q) % NE
            wait_recv(dst.at[i, pl.ds(pl.multiple_of(o * pitch, 16), RB), :], rsem.at[o, i])

    SG = (1, -1)

    def lanes(k, d):
        return pl.ds(d * (W // 2), W // 2) if k == 4 else pl.ds(0, W)

    def z_send(i, k, d, src=None):
        b = (z + NZ - SG[d] * (k - 1)) % NZ
        ref = ZB.at[i, zrow(b), lanes(k, d)]
        remote(
            ref if src is None else src, ref, z_s.at[i], z_r.at[d, k - 1, i], dev(y, (z + NZ + SG[d]) % NZ, c, x)
        ).start()

    def z_wait(i, k, d):
        b = (z + NZ - SG[d] * k) % NZ
        wait_recv(ZB.at[i, zrow(b), lanes(k, d)], z_r.at[d, k - 1, i])

    def r_lanes(k, d):
        return pl.ds(d * (W // 2), W // 2) if k == 1 else pl.ds(0, W)

    def r_send(i, k, d):
        ln = r_lanes(k, d)
        remote(
            RSS.at[i, d, k - 1, :, ln],
            RSR.at[i, d, k - 1, :, ln],
            rs_s.at[i],
            rs_r.at[d, k - 1, i],
            dev(y, (z + NZ + SG[d]) % NZ, c, x),
        ).start()

    def r_wait(i, k, d):
        wait_recv(RSR.at[i, d, k - 1, :, r_lanes(k, d)], rs_r.at[d, k - 1, i])

    def at_chunk(t, lag):
        i = t - lag

        def run(f):
            @pl.when((i >= 0) & (i < NCH))
            def _():
                f(i)

        return run

    def d_rings(p, t, lag):
        for k in (4, 3, 2):
            @at_chunk(t, lag + k - 1)
            def _(i, k=k):
                for d in range(2):
                    z_wait(i, k - 1, d)
                    z_send(i, k, d)

        @at_chunk(t, lag)
        def _(i):
            if p == 0:
                zb_in(i).wait()
            if p == 2:
                @pl.when(i >= H)
                def _():
                    wait_recv(XR.at[i], x_r.at[i])

            for d in range(2):
                z_send(i, 1, d, XR.at[i] if p == 2 else None)
            if p == 2:
                ZB[i, zme, :] = XR[i]

    def d_relay(p, t, lag):
        @at_chunk(t, lag + 5)
        def _(i):
            y_relay(i, RV, RB, rv_r, RL, rl_r, f_s)

    def d_select(p, t, lag):
        @at_chunk(t, lag + 4)
        def _(i):
            for d in range(2):
                z_wait(i, 4, d)
            if p == 2:
                @pl.when(i % H == 0)
                def _():
                    build((x + NX - i // H) % NX, False)
            if p > 0:
                y_sent(i)

            rows = jnp.dot(PM[...], ZB[i], preferred_element_type=F32)
            for n in range(W // 128):
                YS[i, :, n * 128 : (n + 1) * 128] = (rows[:, n * 128 : (n + 1) * 128] * G[...]).astype(BF)
            y_send(i, RV, RB, rv_r, RL, rl_r)

    def d_consume(p, t, lag):
        @at_chunk(t, lag + 6)
        def _(i):
            y_wait(i, RV, RB, rv_r)
            (consume_grad if p == 2 else consume_inner)(i)

    def y_sent(i):
        wait_send(YS.at[i, pl.ds(0, (NE - 1) * RB), :], y_s.at[i])

    def d_sent():
        @pl.loop(0, NCH)
        def _(i):
            wait_send(ZB.at[i, pl.ds(0, (NZ - 1) * T), :], z_s.at[i])
            wait_send(RL.at[i], f_s.at[i])
            y_sent(i)

    def consume_inner(i):
        rows = wide(col(i))

        @pl.loop(0, HID // 256)
        def _(n):
            ln = pl.ds(pl.multiple_of(n * 256, 256), 256)
            IA[:, ln] += jnp.dot(RV[i], DV[rows, ln], preferred_element_type=F32)

    def consume_grad(i):
        xs = (x + NX - i // H) % NX

        @pl.when((i % H == 0) & (i > 0))
        def _():
            wait_recv(AX.at[xs], ax_r.at[xs])

        rows = pl.ds(pl.multiple_of((i % H) * W, W), W)
        IA[rows, :] += lax.dot_general(RV[i], AX[xs], (((0,), (0,)), ((), ())), preferred_element_type=F32)

    def r_final(p, t):
        @at_chunk(t, 6)
        def _(i):
            for d in range(2):
                r_wait(i, 4, d)
            total = PF[i % NPF, zme, :] + RSR[i, 0, 3].astype(F32) + RSR[i, 1, 3].astype(F32)
            term = total.astype(BF)
            if p == 1:
                ZB[i, zme, :] = term
            else:
                lanes_j = wide(col(i))
                grad = (
                    CV[:, lanes_j].astype(F32) + ZB[i, zme, :].astype(F32) + term.astype(F32)
                ).astype(BF)
                ig_ref[:, lanes_j] = grad

                @pl.when(i < H)
                def _():
                    XR[i] = grad

                @pl.when(i >= H)
                def _():
                    XS[i] = grad
                    remote(
                        XS.at[i], XR.at[i], x_s.at[i], x_r.at[i], dev(y, z, c, (x + i // H) % NX)
                    ).start()

    def r_rings(t):
        for k in (4, 3, 2):
            @at_chunk(t, k + 1)
            def _(i, k=k):
                for d in range(2):
                    r_wait(i, k - 1, d)
                    mine = PF.at[i % NPF, zrow((z + NZ + SG[d] * (5 - k)) % NZ), :]
                    if k == 2:
                        half, rest = pl.ds(d * (W // 2), W // 2), pl.ds((1 - d) * (W // 2), W // 2)
                        RSS[i, d, 1, :, rest] = mine[:, rest].astype(BF)
                        RSS[i, d, 1, :, half] = (mine[:, half] + RSR[i, d, 0, :, half].astype(F32)).astype(BF)
                    else:
                        RSS[i, d, k - 1] = (mine[...] + RSR[i, d, k - 2].astype(F32)).astype(BF)
                    r_send(i, k, d)

    def r_relay(t):
        @at_chunk(t, 1)
        def _(i):
            y_relay(i, QV, T, qv_r, QL, ql_r, g_s)

        @at_chunk(t, 3)
        def _(i):
            wait_send(QL.at[i], g_s.at[i])

    def r_combine(t):
        @at_chunk(t, 2)
        def _(i):
            y_wait(i, QV, T, qv_r)
            PF[i % NPF] = jnp.dot(PT[...], QV[i], preferred_element_type=F32)
            for d in range(2):
                ln = pl.ds(d * (W // 2), W // 2)
                RSS[i, d, 0, :, ln] = PF[i % NPF, zrow((z + 4) % NZ), ln].astype(BF)
                r_send(i, 1, d)

    def r_piece(t):
        @at_chunk(t, 0)
        def _(i):
            YS[i] = lax.dot_general(
                SC[...], UV[wide(col(i)), :], (((1,), (1,)), ((), ())), preferred_element_type=F32
            ).astype(BF)
            y_send(i, QV, T, qv_r, QL, ql_r)

    def r_sent():
        @pl.loop(0, NCH)
        def _(i):
            wait_send(ZB.at[i, pl.ds(0, (NZ - 1) * T), :], rs_s.at[i])

    def scale_inner():
        @pl.loop(0, SL // 128)
        def _(n):
            rows = pl.ds(pl.multiple_of(n * 128, 128), 128)
            SC[rows, :] = (IA[rows, :] * SV[rows, :]).astype(BF)
            IA[rows, :] = jnp.zeros((128, HID), F32)

    IA[...] = jnp.zeros_like(IA)

    @pl.loop(0, NCH + 6)
    def _(t):
        d_rings(0, t, 0)

        @pl.when(t == 2)
        def _():
            wait_recv(TGR.at[x, pl.ds(0, NZ - 1)], tg_r.at[x])
            for dx in range(1, NX):
                xs = (x + dx) % NX
                wait_recv(TGR.at[xs], tg_r.at[xs])
            build(x, True)

        @pl.when(t == 0)
        def _():
            ins[1].wait()

        @pl.when(t < NY)
        def _():
            activate(t)

        @pl.when(t == NY)
        def _():
            for copy in ins[2:]:
                copy.wait()
            for dx in range(1, NX):
                remote(AX.at[x], AX.at[x], ax_s.at[0], ax_r.at[x], dev(y, z, c, (x + dx) % NX)).start()

        d_relay(0, t, 0)
        d_select(0, t, 0)
        d_consume(0, t, 0)

    d_sent()

    for p in (1, 2):
        lag = 5 + p
        scale_inner()

        @pl.loop(0, NCH + 6 + lag)
        def _(t, p=p, lag=lag):
            r_final(p, t)
            r_rings(t)
            d_rings(p, t, lag)
            r_relay(t)
            d_relay(p, t, lag)
            r_combine(t)
            d_select(p, t, lag)
            r_piece(t)
            d_consume(p, t, lag)

        r_sent()
        d_sent()

    dg_ref[...] = (IA[: H * W, :] * grad_scale).astype(BF)

    @pl.loop(H, NCH)
    def _(i):
        wait_send(XS.at[i], x_s.at[i])

    for _ in range(NX - 1):
        wait_send(AX.at[x], ax_s.at[0])
    wait_send(TGR.at[pl.ds(0, NX - 1)], tg_s.at[0])
    wait_send(TGR.at[x, pl.ds(0, NZ - 1)], tg_s.at[0])


def body(cotangent, expert_ids, gate_values, hidden_pre, up_weight, down_weight):
    experts = NY * NZ * NC
    onehot = expert_ids[:, :, None] == jnp.arange(experts, dtype=jnp.int32)[None, None, :]
    named = jnp.any(onehot, axis=1)
    count = named.astype(jnp.int32)
    rank = jnp.cumsum(count, axis=0) - count
    rank = jnp.where(named, rank, -1).astype(F32)
    gate = jnp.sum(jnp.where(onehot, gate_values[:, :, None], 0.0), axis=1)

    def planes(table):
        return table.T.reshape(NY, NZ, NC, T).transpose(1, 0, 2, 3).reshape(NZ, NE, T)

    tables = jnp.concatenate([planes(rank), planes(gate)], axis=1)
    vm, dma = pltpu.VMEM, pltpu.SemaphoreType.DMA
    input_grad, down_grad = pl.pallas_call(
        kernel,
        out_shape=(jax.ShapeDtypeStruct((T, D), BF), jax.ShapeDtypeStruct((H * W, HID), BF)),
        in_specs=[pl.BlockSpec(memory_space=pl.ANY)] * 5,
        out_specs=(pl.BlockSpec(memory_space=pltpu.VMEM),) * 2,
        scratch_shapes=[
            vm((T, D), BF),
            vm((NZ, 2 * NE, T), F32),
            vm((NX, NZ, 2 * NE, T), F32),
            vm((SL, HID), BF),
            vm((SL, HID), F32),
            vm((NX, SL, HID), BF),
            vm((D, HID), BF),
            vm((D, HID), BF),
            vm((SL, ZR), BF),
            vm((ZR, NE * T), BF),
            vm((SL, 128), F32),
            vm((NCH, ZR, W), BF),
            vm((NCH, SL, W), BF),
            vm((NCH, 2, RB, W), BF),
            vm((NCH, SL, W), BF),
            vm((NCH, 2, RB, W), BF),
            vm((NCH, NE * T, W), BF),
            vm((SL, HID), F32),
            vm((SL, HID), BF),
            vm((NPF, ZR, W), F32),
            vm((NCH, 2, 4, T, W), BF),
            vm((NCH, 2, 4, T, W), BF),
            vm((NCH, T, W), BF),
            vm((NCH, T, W), BF),
            dma((NCH,)), dma((5,)), dma((1,)), dma((NX,)), dma((1,)), dma((NX,)),
            dma((NCH,)), dma((2, 4, NCH)), dma((NCH,)), dma((2, NCH)), dma((NCH,)), dma((NCH,)), dma((NE, NCH)),
            dma((2, NCH)), dma((NE, NCH)), dma((NCH,)), dma((2, 4, NCH)), dma((NCH,)), dma((NCH,)),
        ],
        compiler_params=pltpu.CompilerParams(has_side_effects=True, vmem_limit_bytes=67043328),
        name="layer",
    )(cotangent, tables, hidden_pre[0], up_weight[0], down_weight[0])
    return (input_grad, down_grad[None])


def solution(mesh):
    in_specs = (
        P(("expert", "token"), None),
        P(("expert", "token"), None),
        P(("expert", "token"), None),
        P("expert", "token", None),
        P("expert", None, None),
        P("expert", None, None),
    )
    out_specs = (P(("expert", "token"), None), P("expert", "token", None))
    return jax.shard_map(body, mesh=mesh, in_specs=in_specs, out_specs=out_specs, check_vma=False)
```

```python
import jax
import jax.numpy as jnp
from jax import lax
from jax.experimental import pallas as pl
from jax.experimental.pallas import tpu as pltpu
from jax.sharding import PartitionSpec as P

grad_scale = 0.03125
root_half = 0.7071067811865476
inv_root_two_pi = 0.3989422804014327

NY, NZ, NC, NX = 4, 8, 2, 4
T = 128
D = 2048
HID = 768
CAP = 14
RB = NZ * CAP
NE = NY * NC
SL = NE * RB
H = 2
NCH = NX * H
W = D // NCH
ZR = NZ * T
NPF = 5
BF = jnp.bfloat16
F32 = jnp.float32
MESH = pl.DeviceIdType.MESH


def slope_and_act(hidden_rows):
    values = hidden_rows
    normal_cdf = 0.5 * (1.0 + lax.erf(values * root_half))
    density = inv_root_two_pi * jnp.exp(-0.5 * values * values)
    slopes = normal_cdf + values * density
    active = (values * normal_cdf).astype(jnp.bfloat16)
    return (slopes, active)


def kernel(
    cot_hbm, id_hbm, gate_hbm, hid_hbm, up_hbm, down_hbm,
    ig_ref, dg_ref,
    CV, IDV, GTV, TV, TGR, HV, SV, AX, UV, DV, PM, PT, G, ZB, YS, RL, RV, QL, QV, IA, SC, PF, RSS, RSR, XS, XR,
    l_zb, l_in, tg_s, tg_r, ax_s, ax_r,
    z_s, z_r, y_s, rl_r, f_s, g_s, rv_r, ql_r, qv_r, rs_s, rs_r, x_s, x_r,
):
    ex = lax.axis_index("expert")
    x = lax.axis_index("token")
    y = ex // (NZ * NC)
    z = (ex // NC) % NZ
    c = ex % NC
    me = y * NC + c
    yp, ym, y2 = (y + 1) % NY, (y + NY - 1) % NY, (y + 2) % NY

    def dev(yy, zz, cc, xx):
        return ((yy * NZ + zz) * NC + cc, xx)

    def remote(src, dst, ssem, rsem, target):
        return pltpu.make_async_remote_copy(
            src_ref=src, dst_ref=dst, send_sem=ssem, recv_sem=rsem, device_id=target, device_id_type=MESH
        )

    partner = dev(y, z, 1 - c, x)

    def wait_recv(ref, rsem):
        remote(ref, ref, tg_s.at[0], rsem, partner).wait_recv()

    def wait_send(ref, ssem):
        remote(ref, ref, ssem, tg_r.at[0], partner).wait_send()

    def col(i):
        return (i + x * H) % NCH

    def wide(j):
        return pl.ds(pl.multiple_of(j * W, W), W)

    def zrow(b):
        return pl.ds(pl.multiple_of(b * T, T), T)

    zme = zrow(z)

    barrier = pltpu.get_barrier_semaphore()

    def greet(target):
        pl.semaphore_signal(barrier, inc=1, device_id=target, device_id_type=MESH)

    @pl.loop(1, NX * NZ)
    def _(q):
        greet(dev(y, (z + q) % NZ, c, (x + q // NZ) % NX))

    for cc in range(NC):
        greet(dev(yp, z, cc, x))
        greet(dev(ym, z, cc, x))
    greet(partner)

    def zb_in(i):
        return pltpu.make_async_copy(cot_hbm.at[:, wide(col(i))], ZB.at[i, zme, :], l_zb.at[i])

    ins = [
        pltpu.make_async_copy(id_hbm, IDV, l_in.at[0]),
        pltpu.make_async_copy(gate_hbm, GTV, l_in.at[1]),
        pltpu.make_async_copy(hid_hbm, HV, l_in.at[2]),
        pltpu.make_async_copy(down_hbm, DV, l_in.at[3]),
        pltpu.make_async_copy(up_hbm, UV, l_in.at[4]),
        pltpu.make_async_copy(cot_hbm, CV, l_in.at[5]),
    ]
    for copy in ins[:3]:
        copy.start()

    @pl.loop(0, NCH)
    def _(i):
        zb_in(i).start()

    for copy in ins[3:]:
        copy.start()

    @pl.loop(0, NCH)
    def _(i):
        for o in range(NE):
            QV[i, o * T + RB : (o + 1) * T, :] = jnp.zeros((T - RB, W), BF)

    IA[...] = jnp.zeros_like(IA)

    def tabulate():
        row = lax.broadcasted_iota(jnp.int32, (NZ * NE, T), 0)
        expert = (((row >> 1) & (NY - 1)) * NZ + (row >> 3)) * NC + (row & (NC - 1))
        named, gate = jnp.zeros((NZ * NE, T), F32), jnp.zeros((NZ * NE, T), F32)
        for k in range(IDV.shape[0]):
            hit = IDV[k : k + 1, :] == expert
            named = jnp.where(hit, 1.0, named)
            gate = jnp.where(hit, GTV[k : k + 1, :], gate)
        first = lax.broadcasted_iota(jnp.int32, (T, T), 0)
        second = lax.broadcasted_iota(jnp.int32, (T, T), 1)
        before = jnp.where(first < second, 1.0, 0.0).astype(BF)
        rank = jnp.dot(named.astype(BF), before, preferred_element_type=F32)
        rank = jnp.where(named > 0.0, rank, -1.0)
        for zz in range(NZ):
            TV[zz, :NE, :] = rank[zz * NE : (zz + 1) * NE]
            TV[zz, NE:, :] = gate[zz * NE : (zz + 1) * NE]

    YB = NZ * NC * CAP

    def activate(b):
        new = lax.broadcasted_iota(jnp.int32, (YB, YB), 0).astype(F32)
        core = jnp.where(new >= float(RB), 1.0, 0.0)
        new = new - core * RB
        plane = jnp.floor((new + 0.5) * (1.0 / CAP))
        old = plane * (NC * CAP) + core * CAP + (new - plane * CAP)
        here = lax.broadcasted_iota(jnp.int32, (YB, YB), 1).astype(F32)
        order = jnp.where(here == old, 1.0, 0.0).astype(BF)
        rows = pl.ds(b * YB, YB)
        hidden = jnp.dot(order, HV[rows, :], preferred_element_type=F32)
        slopes, active = slope_and_act(hidden)
        SV[rows, :] = slopes
        AX[x, rows, :] = active

    def build(xs, with_pt):
        @pl.loop(0, NE)
        def _(o):
            gsum = jnp.zeros((RB, 1), F32)
            rows = pl.ds(pl.multiple_of(o * RB, 16), RB)
            for s in range(NZ):
                rank = TGR[xs, s, pl.ds(o, 1), :]
                gate = TGR[xs, s, pl.ds(NE + o, 1), :]
                slot = jnp.where(rank >= 0.0, rank + float(s * CAP), -1.0)
                iota = lax.broadcasted_iota(jnp.int32, (T, T), 0).astype(F32)
                hit = jnp.where(iota == slot, 1.0, 0.0)
                PM[rows, s * T : (s + 1) * T] = hit[:RB].astype(BF)
                gsum = gsum + jnp.sum(hit[:RB] * gate, axis=1, keepdims=True)
                if with_pt:
                    PT[s * T : (s + 1) * T, pl.ds(pl.multiple_of(o * T, T), T)] = hit.T.astype(BF)
            G[rows, :] = jnp.broadcast_to(gsum, (RB, 128))

    def y_send(i, dst, pitch, rsem, relay, relay_r):
        mine = dst.at[i, pl.ds(pl.multiple_of(me * pitch, 16), RB), :]

        def src(yy, cc):
            return YS.at[i, pl.ds(pl.multiple_of((yy * NC + cc) * RB, 16), RB), :]

        remote(src(y2, 0), relay.at[i, 0], y_s.at[i], relay_r.at[0, i], dev(yp, z, c, x)).start()
        remote(src(y2, 1), relay.at[i, 1], y_s.at[i], relay_r.at[1, i], dev(ym, z, c, x)).start()
        for cc in range(NC):
            remote(src(yp, cc), mine, y_s.at[i], rsem.at[me, i], dev(yp, z, cc, x)).start()
            remote(src(ym, cc), mine, y_s.at[i], rsem.at[me, i], dev(ym, z, cc, x)).start()
        remote(src(y, 1 - c), mine, y_s.at[i], rsem.at[me, i], partner).start()
        dst[i, pl.ds(pl.multiple_of(me * pitch, 16), RB), :] = YS[
            i, pl.ds(pl.multiple_of(me * RB, 16), RB), :
        ]

    def y_relay(i, dst, pitch, rsem, relay, relay_r, fsem):
        for d, (frm, to) in enumerate(((ym, yp), (yp, ym))):
            o = frm * NC + c
            wait_recv(relay.at[i, d], relay_r.at[d, i])
            remote(
                relay.at[i, d],
                dst.at[i, pl.ds(pl.multiple_of(o * pitch, 16), RB), :],
                fsem.at[i],
                rsem.at[o, i],
                dev(to, z, d, x),
            ).start()

    def y_wait(i, dst, pitch, rsem):
        for q in range(1, NE):
            o = (me + q) % NE
            wait_recv(dst.at[i, pl.ds(pl.multiple_of(o * pitch, 16), RB), :], rsem.at[o, i])

    SG = (1, -1)

    def lanes(k, d):
        return pl.ds(d * (W // 2), W // 2) if k == 4 else pl.ds(0, W)

    def z_send(i, k, d, src=None):
        b = (z + NZ - SG[d] * (k - 1)) % NZ
        ref = ZB.at[i, zrow(b), lanes(k, d)]
        remote(
            ref if src is None else src, ref, z_s.at[i], z_r.at[d, k - 1, i], dev(y, (z + NZ + SG[d]) % NZ, c, x)
        ).start()

    def z_wait(i, k, d):
        b = (z + NZ - SG[d] * k) % NZ
        wait_recv(ZB.at[i, zrow(b), lanes(k, d)], z_r.at[d, k - 1, i])

    def r_lanes(k, d):
        return pl.ds(d * (W // 2), W // 2) if k == 1 else pl.ds(0, W)

    def r_send(i, k, d):
        ln = r_lanes(k, d)
        remote(
            RSS.at[i, d, k - 1, :, ln],
            RSR.at[i, d, k - 1, :, ln],
            rs_s.at[i],
            rs_r.at[d, k - 1, i],
            dev(y, (z + NZ + SG[d]) % NZ, c, x),
        ).start()

    def r_wait(i, k, d):
        wait_recv(RSR.at[i, d, k - 1, :, r_lanes(k, d)], rs_r.at[d, k - 1, i])

    def at_chunk(t, lag):
        i = t - lag

        def run(f):
            @pl.when((i >= 0) & (i < NCH))
            def _():
                f(i)

        return run

    def d_ring(p, t, lag, k):
        @at_chunk(t, lag)
        def _(i):
            if k > 1:
                for d in range(2):
                    z_wait(i, k - 1, d)
                    z_send(i, k, d)
                return
            if p == 0:
                zb_in(i).wait()
            if p == 2:
                @pl.when(i >= H)
                def _():
                    wait_recv(XR.at[i], x_r.at[i])

            for d in range(2):
                z_send(i, 1, d, XR.at[i] if p == 2 else None)
            if p == 2:
                ZB[i, zme, :] = XR[i]

    def d_relay(p, t, lag):
        @at_chunk(t, lag)
        def _(i):
            y_relay(i, RV, RB, rv_r, RL, rl_r, f_s)

    def d_select(p, t, lag):
        @at_chunk(t, lag)
        def _(i):
            for d in range(2):
                z_wait(i, 4, d)
            if p == 2:
                @pl.when(i % H == 0)
                def _():
                    build((x + NX - i // H) % NX, False)
            if p > 0:
                y_sent(i)

            rows = jnp.dot(PM[...], ZB[i], preferred_element_type=F32)
            for n in range(W // 128):
                YS[i, :, n * 128 : (n + 1) * 128] = (rows[:, n * 128 : (n + 1) * 128] * G[...]).astype(BF)
            y_send(i, RV, RB, rv_r, RL, rl_r)

    def d_consume(p, t, lag):
        @at_chunk(t, lag)
        def _(i):
            y_wait(i, RV, RB, rv_r)
            (consume_grad if p == 2 else consume_inner)(i)

    def y_sent(i):
        wait_send(YS.at[i, pl.ds(0, (NE - 1) * RB), :], y_s.at[i])

    def d_sent():
        @pl.loop(0, NCH)
        def _(i):
            wait_send(ZB.at[i, pl.ds(0, (NZ - 1) * T), :], z_s.at[i])
            wait_send(RL.at[i], f_s.at[i])
            y_sent(i)

    def consume_inner(i):
        rows = wide(col(i))

        @pl.loop(0, HID // 256)
        def _(n):
            ln = pl.ds(pl.multiple_of(n * 256, 256), 256)
            IA[:, ln] += jnp.dot(RV[i], DV[rows, ln], preferred_element_type=F32)

    def consume_grad(i):
        xs = (x + NX - i // H) % NX

        @pl.when((i % H == 0) & (i > 0))
        def _():
            wait_recv(AX.at[xs], ax_r.at[xs])

        rows = pl.ds(pl.multiple_of((i % H) * W, W), W)
        IA[rows, :] += lax.dot_general(RV[i], AX[xs], (((0,), (0,)), ((), ())), preferred_element_type=F32)

    def r_final(p, t, lag):
        @at_chunk(t, lag)
        def _(i):
            for d in range(2):
                r_wait(i, 4, d)
            total = PF[i % NPF, zme, :] + RSR[i, 0, 3].astype(F32) + RSR[i, 1, 3].astype(F32)
            term = total.astype(BF)
            if p == 1:
                ZB[i, zme, :] = term
            else:
                lanes_j = wide(col(i))
                grad = (
                    CV[:, lanes_j].astype(F32) + ZB[i, zme, :].astype(F32) + term.astype(F32)
                ).astype(BF)
                ig_ref[:, lanes_j] = grad

                @pl.when(i < H)
                def _():
                    XR[i] = grad

                @pl.when(i >= H)
                def _():
                    XS[i] = grad
                    remote(
                        XS.at[i], XR.at[i], x_s.at[i], x_r.at[i], dev(y, z, c, (x + i // H) % NX)
                    ).start()

    def r_ring(t, lag, k):
        @at_chunk(t, lag)
        def _(i):
            for d in range(2):
                r_wait(i, k - 1, d)
                mine = PF.at[i % NPF, zrow((z + NZ + SG[d] * (5 - k)) % NZ), :]
                if k == 2:
                    half, rest = pl.ds(d * (W // 2), W // 2), pl.ds((1 - d) * (W // 2), W // 2)
                    RSS[i, d, 1, :, rest] = mine[:, rest].astype(BF)
                    RSS[i, d, 1, :, half] = (mine[:, half] + RSR[i, d, 0, :, half].astype(F32)).astype(BF)
                else:
                    RSS[i, d, k - 1] = (mine[...] + RSR[i, d, k - 2].astype(F32)).astype(BF)
                r_send(i, k, d)

    def r_relay(t, lag):
        @at_chunk(t, lag)
        def _(i):
            y_relay(i, QV, T, qv_r, QL, ql_r, g_s)

        @at_chunk(t, lag + 2)
        def _(i):
            wait_send(QL.at[i], g_s.at[i])

    def r_combine(t, lag):
        @at_chunk(t, lag)
        def _(i):
            y_wait(i, QV, T, qv_r)
            PF[i % NPF] = jnp.dot(PT[...], QV[i], preferred_element_type=F32)
            for d in range(2):
                ln = pl.ds(d * (W // 2), W // 2)
                RSS[i, d, 0, :, ln] = PF[i % NPF, zrow((z + 4) % NZ), ln].astype(BF)
                r_send(i, 1, d)

    def r_piece(t, lag):
        @at_chunk(t, lag)
        def _(i):
            YS[i] = lax.dot_general(
                SC[...], UV[wide(col(i)), :], (((1,), (1,)), ((), ())), preferred_element_type=F32
            ).astype(BF)
            y_send(i, QV, T, qv_r, QL, ql_r)

    def r_sent():
        @pl.loop(0, NCH)
        def _(i):
            wait_send(ZB.at[i, pl.ds(0, (NZ - 1) * T), :], rs_s.at[i])

    def scale_inner():
        @pl.loop(0, SL // 128)
        def _(n):
            rows = pl.ds(pl.multiple_of(n * 128, 128), 128)
            SC[rows, :] = (IA[rows, :] * SV[rows, :]).astype(BF)
            IA[rows, :] = jnp.zeros((128, HID), F32)

    for copy in ins[:2]:
        copy.wait()
    tabulate()
    ins[2].wait()

    @pl.loop(0, NY)
    def _(b):
        activate(b)

    TGR[x, z] = TV[z]
    pl.semaphore_wait(barrier, NX * NZ - 1 + 2 * NC + 1)

    @pl.loop(0, NCH + 6)
    def _(t):
        for k in (4, 3, 2, 1):
            d_ring(0, t, k - 1, k)

        @pl.when(t == 0)
        def _():
            @pl.loop(1, NX * NZ)
            def _(q):
                xx = (x + q // NZ) % NX
                zz = (z + q) % NZ
                remote(TV.at[zz], TGR.at[x, z], tg_s.at[0], tg_r.at[x], dev(y, zz, c, xx)).start()

        @pl.when(t == 2)
        def _():
            wait_recv(TGR.at[x, pl.ds(0, NZ - 1)], tg_r.at[x])
            build(x, True)

        @pl.when(t == 4)
        def _():
            for dx in range(1, NX):
                xs = (x + dx) % NX
                wait_recv(TGR.at[xs], tg_r.at[xs])
            for copy in ins[3:]:
                copy.wait()
            for dx in range(1, NX):
                remote(AX.at[x], AX.at[x], ax_s.at[0], ax_r.at[x], dev(y, z, c, (x + dx) % NX)).start()

        d_relay(0, t, 4)
        d_select(0, t, 3)
        d_consume(0, t, 6)

    d_sent()

    for p in (1, 2):
        lag = 4 + p
        scale_inner()

        @pl.loop(0, NCH + 5 + lag)
        def _(t, p=p, lag=lag):
            r_relay(t, 1)
            r_final(p, t, 5)
            d_ring(p, t, lag + 3, 4)
            d_ring(p, t, lag + 2, 3)
            r_ring(t, 4, 4)
            r_piece(t, 0)
            d_consume(p, t, lag + 5)
            d_ring(p, t, lag + 1, 2)
            r_ring(t, 3, 3)
            d_ring(p, t, lag, 1)
            r_ring(t, 2, 2)
            d_relay(p, t, lag + 4)
            d_select(p, t, lag + 3)
            r_combine(t, 1)

        r_sent()
        d_sent()

    dg_ref[...] = (IA[: H * W, :] * grad_scale).astype(BF)

    @pl.loop(H, NCH)
    def _(i):
        wait_send(XS.at[i], x_s.at[i])

    for _ in range(NX - 1):
        wait_send(AX.at[x], ax_s.at[0])
    wait_send(TGR.at[pl.ds(0, NX - 1)], tg_s.at[0])
    wait_send(TGR.at[x, pl.ds(0, NZ - 1)], tg_s.at[0])


def body(cotangent, expert_ids, gate_values, hidden_pre, up_weight, down_weight):
    vm, dma = pltpu.VMEM, pltpu.SemaphoreType.DMA
    input_grad, down_grad = pl.pallas_call(
        kernel,
        out_shape=(jax.ShapeDtypeStruct((T, D), BF), jax.ShapeDtypeStruct((H * W, HID), BF)),
        in_specs=[pl.BlockSpec(memory_space=pl.ANY)] * 6,
        out_specs=(pl.BlockSpec(memory_space=pltpu.VMEM),) * 2,
        scratch_shapes=[
            vm((T, D), BF),
            vm(expert_ids.shape[::-1], jnp.int32),
            vm(gate_values.shape[::-1], F32),
            vm((NZ, 2 * NE, T), F32),
            vm((NX, NZ, 2 * NE, T), F32),
            vm((SL, HID), BF),
            vm((SL, HID), F32),
            vm((NX, SL, HID), BF),
            vm((D, HID), BF),
            vm((D, HID), BF),
            vm((SL, ZR), BF),
            vm((ZR, NE * T), BF),
            vm((SL, 128), F32),
            vm((NCH, ZR, W), BF),
            vm((NCH, SL, W), BF),
            vm((NCH, 2, RB, W), BF),
            vm((NCH, SL, W), BF),
            vm((NCH, 2, RB, W), BF),
            vm((NCH, NE * T, W), BF),
            vm((SL, HID), F32),
            vm((SL, HID), BF),
            vm((NPF, ZR, W), F32),
            vm((NCH, 2, 4, T, W), BF),
            vm((NCH, 2, 4, T, W), BF),
            vm((NCH, T, W), BF),
            vm((NCH, T, W), BF),
            dma((NCH,)), dma((6,)), dma((1,)), dma((NX,)), dma((1,)), dma((NX,)),
            dma((NCH,)), dma((2, 4, NCH)), dma((NCH,)), dma((2, NCH)), dma((NCH,)), dma((NCH,)), dma((NE, NCH)),
            dma((2, NCH)), dma((NE, NCH)), dma((NCH,)), dma((2, 4, NCH)), dma((NCH,)), dma((NCH,)),
        ],
        compiler_params=pltpu.CompilerParams(has_side_effects=True, collective_id=0, vmem_limit_bytes=67043328),
        name="layer",
    )(cotangent, expert_ids.T, gate_values.T, hidden_pre[0], up_weight[0], down_weight[0])
    return (input_grad, down_grad[None])


def solution(mesh):
    in_specs = (
        P(("expert", "token"), None),
        P(("expert", "token"), None),
        P(("expert", "token"), None),
        P("expert", "token", None),
        P("expert", None, None),
        P("expert", None, None),
    )
    out_specs = (P(("expert", "token"), None), P("expert", "token", None))
    return jax.shard_map(body, mesh=mesh, in_specs=in_specs, out_specs=out_specs, check_vma=False)
```

```python
import jax
import jax.numpy as jnp
from jax import lax
from jax.experimental import pallas as pl
from jax.experimental.pallas import tpu as pltpu
from jax.sharding import PartitionSpec as P

grad_scale = 0.03125
root_half = 0.7071067811865476
inv_root_two_pi = 0.3989422804014327

NY, NZ, NC, NX = 4, 8, 2, 4
T = 128
D = 2048
HID = 768
CAP = 14
RB = NZ * CAP
NE = NY * NC
SL = NE * RB
H = 2
NCH = NX * H
W = D // NCH
ZR = NZ * T
NPF = 5
BF = jnp.bfloat16
F32 = jnp.float32
MESH = pl.DeviceIdType.MESH


def slope_and_act(hidden_rows):
    values = hidden_rows
    normal_cdf = 0.5 * (1.0 + lax.erf(values * root_half))
    density = inv_root_two_pi * jnp.exp(-0.5 * values * values)
    slopes = normal_cdf + values * density
    active = (values * normal_cdf).astype(jnp.bfloat16)
    return (slopes, active)


def kernel(
    cot_hbm, id_hbm, gate_hbm, hid_hbm, up_hbm, down_hbm,
    ig_ref, dg_ref,
    CV, IDV, GTV, TV, TGR, HV, SV, AX, UV, DV, PM, PT, G, ZB, YS, RV, QV, IA, SC, PF, RSS, RSR, XS, XR,
    l_zb, l_in, tg_s, tg_r, ax_s, ax_r,
    z_s, z_r, y_s, rv_r, qv_r, rs_s, rs_r, x_s, x_r,
):
    ex = lax.axis_index("expert")
    x = lax.axis_index("token")
    y = ex // (NZ * NC)
    z = (ex // NC) % NZ
    c = ex % NC
    me = y * NC + c
    yp, ym, y2 = (y + 1) % NY, (y + NY - 1) % NY, (y + 2) % NY

    def dev(yy, zz, cc, xx):
        return ((yy * NZ + zz) * NC + cc, xx)

    def remote(src, dst, ssem, rsem, target):
        return pltpu.make_async_remote_copy(
            src_ref=src, dst_ref=dst, send_sem=ssem, recv_sem=rsem, device_id=target, device_id_type=MESH
        )

    partner = dev(y, z, 1 - c, x)

    def wait_recv(ref, rsem):
        remote(ref, ref, tg_s.at[0], rsem, partner).wait_recv()

    def wait_send(ref, ssem):
        remote(ref, ref, ssem, tg_r.at[0], partner).wait_send()

    def col(i):
        return (i + x * H) % NCH

    def wide(j):
        return pl.ds(pl.multiple_of(j * W, W), W)

    def zrow(b):
        return pl.ds(pl.multiple_of(b * T, T), T)

    zme = zrow(z)

    barrier = pltpu.get_barrier_semaphore()

    def greet(target):
        pl.semaphore_signal(barrier, inc=1, device_id=target, device_id_type=MESH)

    @pl.loop(1, NX * NZ)
    def _(q):
        greet(dev(y, (z + q) % NZ, c, (x + q // NZ) % NX))

    for cc in range(NC):
        greet(dev(y2, z, cc, x))
        greet(dev(yp, z, cc, x))
        greet(dev(ym, z, cc, x))
    greet(partner)

    def zb_in(i):
        return pltpu.make_async_copy(cot_hbm.at[:, wide(col(i))], ZB.at[i, zme, :], l_zb.at[i])

    ins = [
        pltpu.make_async_copy(id_hbm, IDV, l_in.at[0]),
        pltpu.make_async_copy(gate_hbm, GTV, l_in.at[1]),
        pltpu.make_async_copy(hid_hbm, HV, l_in.at[2]),
        pltpu.make_async_copy(down_hbm, DV, l_in.at[3]),
        pltpu.make_async_copy(up_hbm, UV, l_in.at[4]),
        pltpu.make_async_copy(cot_hbm, CV, l_in.at[5]),
    ]
    for copy in ins[:3]:
        copy.start()

    @pl.loop(0, NCH)
    def _(i):
        zb_in(i).start()

    for copy in ins[3:]:
        copy.start()

    @pl.loop(0, NCH)
    def _(i):
        for o in range(NE):
            QV[i, o * T + RB : (o + 1) * T, :] = jnp.zeros((T - RB, W), BF)

    IA[...] = jnp.zeros_like(IA)

    def tabulate():
        row = lax.broadcasted_iota(jnp.int32, (NZ * NE, T), 0)
        expert = (((row >> 1) & (NY - 1)) * NZ + (row >> 3)) * NC + (row & (NC - 1))
        named, gate = jnp.zeros((NZ * NE, T), F32), jnp.zeros((NZ * NE, T), F32)
        for k in range(IDV.shape[0]):
            hit = IDV[k : k + 1, :] == expert
            named = jnp.where(hit, 1.0, named)
            gate = jnp.where(hit, GTV[k : k + 1, :], gate)
        first = lax.broadcasted_iota(jnp.int32, (T, T), 0)
        second = lax.broadcasted_iota(jnp.int32, (T, T), 1)
        before = jnp.where(first < second, 1.0, 0.0).astype(BF)
        rank = jnp.dot(named.astype(BF), before, preferred_element_type=F32)
        rank = jnp.where(named > 0.0, rank, -1.0)
        for zz in range(NZ):
            TV[zz, :NE, :] = rank[zz * NE : (zz + 1) * NE]
            TV[zz, NE:, :] = gate[zz * NE : (zz + 1) * NE]

    YB = NZ * NC * CAP

    def activate(b):
        new = lax.broadcasted_iota(jnp.int32, (YB, YB), 0).astype(F32)
        core = jnp.where(new >= float(RB), 1.0, 0.0)
        new = new - core * RB
        plane = jnp.floor((new + 0.5) * (1.0 / CAP))
        old = plane * (NC * CAP) + core * CAP + (new - plane * CAP)
        here = lax.broadcasted_iota(jnp.int32, (YB, YB), 1).astype(F32)
        order = jnp.where(here == old, 1.0, 0.0).astype(BF)
        rows = pl.ds(b * YB, YB)
        hidden = jnp.dot(order, HV[rows, :], preferred_element_type=F32)
        slopes, active = slope_and_act(hidden)
        SV[rows, :] = slopes
        AX[x, rows, :] = active

    def build(xs, with_pt):
        @pl.loop(0, NE)
        def _(o):
            gsum = jnp.zeros((RB, 1), F32)
            rows = pl.ds(pl.multiple_of(o * RB, 16), RB)
            for s in range(NZ):
                rank = TGR[xs, s, pl.ds(o, 1), :]
                gate = TGR[xs, s, pl.ds(NE + o, 1), :]
                slot = jnp.where(rank >= 0.0, rank + float(s * CAP), -1.0)
                iota = lax.broadcasted_iota(jnp.int32, (T, T), 0).astype(F32)
                hit = jnp.where(iota == slot, 1.0, 0.0)
                PM[rows, s * T : (s + 1) * T] = hit[:RB].astype(BF)
                gsum = gsum + jnp.sum(hit[:RB] * gate, axis=1, keepdims=True)
                if with_pt:
                    PT[s * T : (s + 1) * T, pl.ds(pl.multiple_of(o * T, T), T)] = hit.T.astype(BF)
            G[rows, :] = jnp.broadcast_to(gsum, (RB, 128))

    def y_send(i, dst, pitch, rsem):
        mine = dst.at[i, pl.ds(pl.multiple_of(me * pitch, 16), RB), :]

        def src(yy, cc):
            return YS.at[i, pl.ds(pl.multiple_of((yy * NC + cc) * RB, 16), RB), :]

        for cc in range(NC):
            remote(src(y2, cc), mine, y_s.at[i], rsem.at[me, i], dev(y2, z, cc, x)).start()
        for cc in range(NC):
            remote(src(yp, cc), mine, y_s.at[i], rsem.at[me, i], dev(yp, z, cc, x)).start()
            remote(src(ym, cc), mine, y_s.at[i], rsem.at[me, i], dev(ym, z, cc, x)).start()
        remote(src(y, 1 - c), mine, y_s.at[i], rsem.at[me, i], partner).start()
        dst[i, pl.ds(pl.multiple_of(me * pitch, 16), RB), :] = YS[
            i, pl.ds(pl.multiple_of(me * RB, 16), RB), :
        ]

    def y_wait(i, dst, pitch, rsem):
        for q in range(1, NE):
            o = (me + q) % NE
            wait_recv(dst.at[i, pl.ds(pl.multiple_of(o * pitch, 16), RB), :], rsem.at[o, i])

    SG = (1, -1)

    HT = T // 2

    def z_ref(i, b, k, d):
        rows = pl.ds(pl.multiple_of(b * T + d * HT, HT), HT) if k == 4 else zrow(b)
        return ZB.at[i, rows, :]

    def z_send(i, k, d, src=None):
        ref = z_ref(i, (z + NZ - SG[d] * (k - 1)) % NZ, k, d)
        remote(
            ref if src is None else src, ref, z_s.at[i], z_r.at[d, k - 1, i], dev(y, (z + NZ + SG[d]) % NZ, c, x)
        ).start()

    def z_wait(i, k, d):
        wait_recv(z_ref(i, (z + NZ - SG[d] * k) % NZ, k, d), z_r.at[d, k - 1, i])

    def r_rows(k, d):
        return pl.ds(d * HT, HT) if k == 1 else pl.ds(0, T)

    def r_send(i, k, d):
        rows = r_rows(k, d)
        remote(
            RSS.at[i, d, k - 1, rows, :],
            RSR.at[i, d, k - 1, rows, :],
            rs_s.at[i],
            rs_r.at[d, k - 1, i],
            dev(y, (z + NZ + SG[d]) % NZ, c, x),
        ).start()

    def r_wait(i, k, d):
        wait_recv(RSR.at[i, d, k - 1, r_rows(k, d), :], rs_r.at[d, k - 1, i])

    def at_chunk(t, lag):
        i = t - lag

        def run(f):
            @pl.when((i >= 0) & (i < NCH))
            def _():
                f(i)

        return run

    def d_ring(p, t, lag, k):
        @at_chunk(t, lag)
        def _(i):
            if k > 1:
                for d in range(2):
                    z_wait(i, k - 1, d)
                    z_send(i, k, d)
                return
            if p == 0:
                zb_in(i).wait()
            if p == 2:
                @pl.when(i >= H)
                def _():
                    wait_recv(XR.at[i], x_r.at[i])

            for d in range(2):
                z_send(i, 1, d, XR.at[i] if p == 2 else None)
            if p == 2:
                ZB[i, zme, :] = XR[i]

    def d_select(p, t, lag):
        @at_chunk(t, lag)
        def _(i):
            for d in range(2):
                z_wait(i, 4, d)
            if p == 2:
                @pl.when(i % H == 0)
                def _():
                    build((x + NX - i // H) % NX, False)
            if p > 0:
                y_sent(i)

            rows = jnp.dot(PM[...], ZB[i], preferred_element_type=F32)
            for n in range(W // 128):
                YS[i, :, n * 128 : (n + 1) * 128] = (rows[:, n * 128 : (n + 1) * 128] * G[...]).astype(BF)
            y_send(i, RV, RB, rv_r)

    def d_consume(p, t, lag):
        @at_chunk(t, lag)
        def _(i):
            y_wait(i, RV, RB, rv_r)
            (consume_grad if p == 2 else consume_inner)(i)

    def y_sent(i):
        wait_send(YS.at[i, pl.ds(0, (NE - 1) * RB), :], y_s.at[i])

    def d_sent():
        @pl.loop(0, NCH)
        def _(i):
            wait_send(ZB.at[i, pl.ds(0, (NZ - 1) * T), :], z_s.at[i])
            y_sent(i)

    def consume_inner(i):
        rows = wide(col(i))

        @pl.loop(0, HID // 256)
        def _(n):
            ln = pl.ds(pl.multiple_of(n * 256, 256), 256)
            IA[:, ln] += jnp.dot(RV[i], DV[rows, ln], preferred_element_type=F32)

    def consume_grad(i):
        xs = (x + NX - i // H) % NX

        @pl.when((i % H == 0) & (i > 0))
        def _():
            wait_recv(AX.at[xs], ax_r.at[xs])

        rows = pl.ds(pl.multiple_of((i % H) * W, W), W)
        IA[rows, :] += lax.dot_general(RV[i], AX[xs], (((0,), (0,)), ((), ())), preferred_element_type=F32)

    def r_final(p, t, lag):
        @at_chunk(t, lag)
        def _(i):
            for d in range(2):
                r_wait(i, 4, d)
            total = PF[i % NPF, zme, :] + RSR[i, 0, 3].astype(F32) + RSR[i, 1, 3].astype(F32)
            term = total.astype(BF)
            if p == 1:
                ZB[i, zme, :] = term
            else:
                lanes_j = wide(col(i))
                grad = (
                    CV[:, lanes_j].astype(F32) + ZB[i, zme, :].astype(F32) + term.astype(F32)
                ).astype(BF)
                ig_ref[:, lanes_j] = grad

                @pl.when(i < H)
                def _():
                    XR[i] = grad

                @pl.when(i >= H)
                def _():
                    XS[i] = grad
                    remote(
                        XS.at[i], XR.at[i], x_s.at[i], x_r.at[i], dev(y, z, c, (x + i // H) % NX)
                    ).start()

    def r_ring(t, lag, k):
        @at_chunk(t, lag)
        def _(i):
            for d in range(2):
                r_wait(i, k - 1, d)
                mine = PF.at[i % NPF, zrow((z + NZ + SG[d] * (5 - k)) % NZ), :]
                if k == 2:
                    half, rest = pl.ds(d * HT, HT), pl.ds((1 - d) * HT, HT)
                    RSS[i, d, 1, rest, :] = mine[rest, :].astype(BF)
                    RSS[i, d, 1, half, :] = (mine[half, :] + RSR[i, d, 0, half, :].astype(F32)).astype(BF)
                else:
                    RSS[i, d, k - 1] = (mine[...] + RSR[i, d, k - 2].astype(F32)).astype(BF)
                r_send(i, k, d)

    def r_combine(t, lag):
        @at_chunk(t, lag)
        def _(i):
            y_wait(i, QV, T, qv_r)
            PF[i % NPF] = jnp.dot(PT[...], QV[i], preferred_element_type=F32)
            for d in range(2):
                far = pl.ds(pl.multiple_of((z + 4) % NZ * T + d * HT, HT), HT)
                RSS[i, d, 0, d * HT : (d + 1) * HT, :] = PF[i % NPF, far, :].astype(BF)
                r_send(i, 1, d)

    def r_piece(t, lag):
        @at_chunk(t, lag)
        def _(i):
            YS[i] = lax.dot_general(
                SC[...], UV[wide(col(i)), :], (((1,), (1,)), ((), ())), preferred_element_type=F32
            ).astype(BF)
            y_send(i, QV, T, qv_r)

    def r_sent():
        @pl.loop(0, NCH)
        def _(i):
            wait_send(ZB.at[i, pl.ds(0, (NZ - 1) * T), :], rs_s.at[i])

    def scale_inner():
        @pl.loop(0, SL // 128)
        def _(n):
            rows = pl.ds(pl.multiple_of(n * 128, 128), 128)
            SC[rows, :] = (IA[rows, :] * SV[rows, :]).astype(BF)
            IA[rows, :] = jnp.zeros((128, HID), F32)

    for copy in ins[:2]:
        copy.wait()
    tabulate()
    ins[2].wait()

    @pl.loop(0, NY)
    def _(b):
        activate(b)

    TGR[x, z] = TV[z]
    pl.semaphore_wait(barrier, NX * NZ - 1 + 3 * NC + 1)

    @pl.loop(0, NCH + 4)
    def _(t):
        for k in (4, 3, 2, 1):
            d_ring(0, t, k - 1, k)

        @pl.when(t == 0)
        def _():
            @pl.loop(1, NX * NZ)
            def _(q):
                xx = (x + q // NZ) % NX
                zz = (z + q) % NZ
                remote(TV.at[zz], TGR.at[x, z], tg_s.at[0], tg_r.at[x], dev(y, zz, c, xx)).start()

        @pl.when(t == 2)
        def _():
            wait_recv(TGR.at[x, pl.ds(0, NZ - 1)], tg_r.at[x])
            build(x, True)

        @pl.when(t == 4)
        def _():
            for dx in range(1, NX):
                xs = (x + dx) % NX
                wait_recv(TGR.at[xs], tg_r.at[xs])
            for copy in ins[3:]:
                copy.wait()
            for dx in range(1, NX):
                remote(AX.at[x], AX.at[x], ax_s.at[0], ax_r.at[x], dev(y, z, c, (x + dx) % NX)).start()

        d_select(0, t, 3)
        d_consume(0, t, 4)

    d_sent()

    for p in (1, 2):
        lag = 4 + p
        scale_inner()

        @pl.loop(0, NCH + 4 + lag)
        def _(t, p=p, lag=lag):
            r_final(p, t, 5)
            d_ring(p, t, lag + 3, 4)
            d_ring(p, t, lag + 2, 3)
            r_ring(t, 4, 4)
            r_piece(t, 0)
            d_consume(p, t, lag + 4)
            d_ring(p, t, lag + 1, 2)
            r_ring(t, 3, 3)
            d_ring(p, t, lag, 1)
            r_ring(t, 2, 2)
            d_select(p, t, lag + 3)
            r_combine(t, 1)

        r_sent()
        d_sent()

    dg_ref[...] = (IA[: H * W, :] * grad_scale).astype(BF)

    @pl.loop(H, NCH)
    def _(i):
        wait_send(XS.at[i], x_s.at[i])

    for _ in range(NX - 1):
        wait_send(AX.at[x], ax_s.at[0])
    wait_send(TGR.at[pl.ds(0, NX - 1)], tg_s.at[0])
    wait_send(TGR.at[x, pl.ds(0, NZ - 1)], tg_s.at[0])


def hand_over(a_ref, b_ref, c_ref, d_ref):
    c_ref[...] = a_ref[...]
    d_ref[...] = b_ref[...]


def body(cotangent, expert_ids, gate_values, hidden_pre, up_weight, down_weight):
    vm, dma = pltpu.VMEM, pltpu.SemaphoreType.DMA
    input_grad, down_grad = pl.pallas_call(
        kernel,
        out_shape=(jax.ShapeDtypeStruct((T, D), BF), jax.ShapeDtypeStruct((H * W, HID), BF)),
        in_specs=[pl.BlockSpec(memory_space=pl.ANY)] * 6,
        out_specs=(pl.BlockSpec(memory_space=pltpu.VMEM),) * 2,
        scratch_shapes=[
            vm((T, D), BF),
            vm(expert_ids.shape[::-1], jnp.int32),
            vm(gate_values.shape[::-1], F32),
            vm((NZ, 2 * NE, T), F32),
            vm((NX, NZ, 2 * NE, T), F32),
            vm((SL, HID), BF),
            vm((SL, HID), F32),
            vm((NX, SL, HID), BF),
            vm((D, HID), BF),
            vm((D, HID), BF),
            vm((SL, ZR), BF),
            vm((ZR, NE * T), BF),
            vm((SL, 128), F32),
            vm((NCH, ZR, W), BF),
            vm((NCH, SL, W), BF),
            vm((NCH, SL, W), BF),
            vm((NCH, NE * T, W), BF),
            vm((SL, HID), F32),
            vm((SL, HID), BF),
            vm((NPF, ZR, W), F32),
            vm((NCH, 2, 4, T, W), BF),
            vm((NCH, 2, 4, T, W), BF),
            vm((NCH, T, W), BF),
            vm((NCH, T, W), BF),
            dma((NCH,)), dma((6,)), dma((1,)), dma((NX,)), dma((1,)), dma((NX,)),
            dma((NCH,)), dma((2, 4, NCH)), dma((NCH,)), dma((NE, NCH)), dma((NE, NCH)),
            dma((NCH,)), dma((2, 4, NCH)), dma((NCH,)), dma((NCH,)),
        ],
        compiler_params=pltpu.CompilerParams(has_side_effects=True, collective_id=0, vmem_limit_bytes=67043328),
        name="layer",
    )(cotangent, expert_ids.T, gate_values.T, hidden_pre[0], up_weight[0], down_weight[0])
    input_grad, down_grad = pl.pallas_call(
        hand_over,
        out_shape=(jax.ShapeDtypeStruct((T, D), BF), jax.ShapeDtypeStruct((H * W, HID), BF)),
        in_specs=[pl.BlockSpec(memory_space=pltpu.VMEM)] * 2,
        out_specs=(pl.BlockSpec(memory_space=pltpu.VMEM),) * 2,
        name="hand_over",
    )(input_grad, down_grad)
    return (input_grad, down_grad[None])


def solution(mesh):
    in_specs = (
        P(("expert", "token"), None),
        P(("expert", "token"), None),
        P(("expert", "token"), None),
        P("expert", "token", None),
        P("expert", None, None),
        P("expert", None, None),
    )
    out_specs = (P(("expert", "token"), None), P("expert", "token", None))
    return jax.shard_map(body, mesh=mesh, in_specs=in_specs, out_specs=out_specs, check_vma=False)
```

```python
import jax
import jax.numpy as jnp
from jax import lax
from jax.experimental import pallas as pl
from jax.experimental.pallas import tpu as pltpu
from jax.sharding import PartitionSpec as P

grad_scale = 0.03125
root_half = 0.7071067811865476
inv_root_two_pi = 0.3989422804014327

NY, NZ, NC, NX = 4, 8, 2, 4
T = 128
D = 2048
HID = 768
CAP = 14
RB = NZ * CAP
NE = NY * NC
SL = NE * RB
H = 2
NCH = NX * H
W = D // NCH
ZR = NZ * T
NPF = 5
BF = jnp.bfloat16
F32 = jnp.float32
MESH = pl.DeviceIdType.MESH


def slope_and_act(hidden_rows):
    values = hidden_rows
    normal_cdf = 0.5 * (1.0 + lax.erf(values * root_half))
    density = inv_root_two_pi * jnp.exp(-0.5 * values * values)
    slopes = normal_cdf + values * density
    active = (values * normal_cdf).astype(jnp.bfloat16)
    return (slopes, active)


def kernel(
    cot_hbm, id_hbm, gate_hbm, hid_hbm, up_hbm, down_hbm,
    ig_ref, dg_ref,
    CV, IDV, GTV, TV, TGR, HV, SV, AX, UV, DV, PM, PT, G, ZB, YS, RV, QV, IA, SC, PF, RSS, RSR, XS, XR,
    l_zb, l_in, tg_s, tg_r, ax_s, ax_r,
    z_s, z_r, y_s, rv_r, qv_r, rs_s, rs_r, x_s, x_r,
):
    ex = lax.axis_index("expert")
    x = lax.axis_index("token")
    y = ex // (NZ * NC)
    z = (ex // NC) % NZ
    c = ex % NC
    me = y * NC + c
    yp, ym, y2 = (y + 1) % NY, (y + NY - 1) % NY, (y + 2) % NY

    def dev(yy, zz, cc, xx):
        return ((yy * NZ + zz) * NC + cc, xx)

    def remote(src, dst, ssem, rsem, target):
        return pltpu.make_async_remote_copy(
            src_ref=src, dst_ref=dst, send_sem=ssem, recv_sem=rsem, device_id=target, device_id_type=MESH
        )

    partner = dev(y, z, 1 - c, x)

    def wait_recv(ref, rsem):
        remote(ref, ref, tg_s.at[0], rsem, partner).wait_recv()

    def wait_send(ref, ssem):
        remote(ref, ref, ssem, tg_r.at[0], partner).wait_send()

    def col(i):
        return (i + x * H) % NCH

    def wide(j):
        return pl.ds(pl.multiple_of(j * W, W), W)

    def zrow(b):
        return pl.ds(pl.multiple_of(b * T, T), T)

    zme = zrow(z)

    barrier = pltpu.get_barrier_semaphore()

    def greet(target):
        pl.semaphore_signal(barrier, inc=1, device_id=target, device_id_type=MESH)

    @pl.loop(1, NX * NZ)
    def _(q):
        greet(dev(y, (z + q) % NZ, c, (x + q // NZ) % NX))

    for cc in range(NC):
        greet(dev(y2, z, cc, x))
        greet(dev(yp, z, cc, x))
        greet(dev(ym, z, cc, x))
    greet(partner)

    def zb_in(i):
        return pltpu.make_async_copy(cot_hbm.at[:, wide(col(i))], ZB.at[i, zme, :], l_zb.at[i])

    ins = [
        pltpu.make_async_copy(id_hbm, IDV, l_in.at[0]),
        pltpu.make_async_copy(gate_hbm, GTV, l_in.at[1]),
        pltpu.make_async_copy(hid_hbm, HV, l_in.at[2]),
        pltpu.make_async_copy(down_hbm, DV, l_in.at[3]),
        pltpu.make_async_copy(up_hbm, UV, l_in.at[4]),
        pltpu.make_async_copy(cot_hbm, CV, l_in.at[5]),
    ]
    for copy in ins[:3]:
        copy.start()

    @pl.loop(0, NCH)
    def _(i):
        zb_in(i).start()

    for copy in ins[3:]:
        copy.start()

    @pl.loop(0, NCH)
    def _(i):
        for o in range(NE):
            QV[i, o * T + RB : (o + 1) * T, :] = jnp.zeros((T - RB, W), BF)

    IA[...] = jnp.zeros_like(IA)

    def tabulate():
        row = lax.broadcasted_iota(jnp.int32, (NZ * NE, T), 0)
        expert = (((row >> 1) & (NY - 1)) * NZ + (row >> 3)) * NC + (row & (NC - 1))
        named, gate = jnp.zeros((NZ * NE, T), F32), jnp.zeros((NZ * NE, T), F32)
        for k in range(IDV.shape[0]):
            hit = IDV[k : k + 1, :] == expert
            named = jnp.where(hit, 1.0, named)
            gate = jnp.where(hit, GTV[k : k + 1, :], gate)
        first = lax.broadcasted_iota(jnp.int32, (T, T), 0)
        second = lax.broadcasted_iota(jnp.int32, (T, T), 1)
        before = jnp.where(first < second, 1.0, 0.0).astype(BF)
        rank = jnp.dot(named.astype(BF), before, preferred_element_type=F32)
        rank = jnp.where(named > 0.0, rank, -1.0)
        for zz in range(NZ):
            TV[zz, :NE, :] = rank[zz * NE : (zz + 1) * NE]
            TV[zz, NE:, :] = gate[zz * NE : (zz + 1) * NE]

    YB = NZ * NC * CAP

    def activate(b):
        new = lax.broadcasted_iota(jnp.int32, (YB, YB), 0).astype(F32)
        core = jnp.where(new >= float(RB), 1.0, 0.0)
        new = new - core * RB
        plane = jnp.floor((new + 0.5) * (1.0 / CAP))
        old = plane * (NC * CAP) + core * CAP + (new - plane * CAP)
        here = lax.broadcasted_iota(jnp.int32, (YB, YB), 1).astype(F32)
        order = jnp.where(here == old, 1.0, 0.0).astype(BF)
        rows = pl.ds(b * YB, YB)
        hidden = jnp.dot(order, HV[rows, :], preferred_element_type=F32)
        slopes, active = slope_and_act(hidden)
        SV[rows, :] = slopes
        AX[x, rows, :] = active

    def build(xs, with_pt):
        @pl.loop(0, NE)
        def _(o):
            gsum = jnp.zeros((RB, 1), F32)
            rows = pl.ds(pl.multiple_of(o * RB, 16), RB)
            for s in range(NZ):
                rank = TGR[xs, s, pl.ds(o, 1), :]
                gate = TGR[xs, s, pl.ds(NE + o, 1), :]
                slot = jnp.where(rank >= 0.0, rank + float(s * CAP), -1.0)
                iota = lax.broadcasted_iota(jnp.int32, (T, T), 0).astype(F32)
                hit = jnp.where(iota == slot, 1.0, 0.0)
                PM[rows, s * T : (s + 1) * T] = hit[:RB].astype(BF)
                gsum = gsum + jnp.sum(hit[:RB] * gate, axis=1, keepdims=True)
                if with_pt:
                    PT[s * T : (s + 1) * T, pl.ds(pl.multiple_of(o * T, T), T)] = hit.T.astype(BF)
            G[rows, :] = jnp.broadcast_to(gsum, (RB, 128))

    def y_send(i, dst, pitch, rsem):
        mine = dst.at[i, pl.ds(pl.multiple_of(me * pitch, 16), RB), :]

        def src(yy, cc):
            return YS.at[i, pl.ds(pl.multiple_of((yy * NC + cc) * RB, 16), RB), :]

        for cc in range(NC):
            remote(src(y2, cc), mine, y_s.at[i], rsem.at[me, i], dev(y2, z, cc, x)).start()
        for cc in range(NC):
            remote(src(yp, cc), mine, y_s.at[i], rsem.at[me, i], dev(yp, z, cc, x)).start()
            remote(src(ym, cc), mine, y_s.at[i], rsem.at[me, i], dev(ym, z, cc, x)).start()
        remote(src(y, 1 - c), mine, y_s.at[i], rsem.at[me, i], partner).start()
        dst[i, pl.ds(pl.multiple_of(me * pitch, 16), RB), :] = YS[
            i, pl.ds(pl.multiple_of(me * RB, 16), RB), :
        ]

    def y_wait(i, dst, pitch, rsem):
        for q in range(1, NE):
            o = (me + q) % NE
            wait_recv(dst.at[i, pl.ds(pl.multiple_of(o * pitch, 16), RB), :], rsem.at[o, i])

    SG = (1, -1)

    HT = T // 2

    def z_ref(i, b, k, d):
        rows = pl.ds(pl.multiple_of(b * T + d * HT, HT), HT) if k == 4 else zrow(b)
        return ZB.at[i, rows, :]

    def z_send(i, k, d, src=None):
        ref = z_ref(i, (z + NZ - SG[d] * (k - 1)) % NZ, k, d)
        remote(
            ref if src is None else src, ref, z_s.at[i], z_r.at[d, k - 1, i], dev(y, (z + NZ + SG[d]) % NZ, c, x)
        ).start()

    def z_wait(i, k, d):
        wait_recv(z_ref(i, (z + NZ - SG[d] * k) % NZ, k, d), z_r.at[d, k - 1, i])

    def r_rows(k, d):
        return pl.ds(d * HT, HT) if k == 1 else pl.ds(0, T)

    def r_send(i, k, d):
        rows = r_rows(k, d)
        remote(
            RSS.at[i, d, k - 1, rows, :],
            RSR.at[i, d, k - 1, rows, :],
            rs_s.at[i],
            rs_r.at[d, k - 1, i],
            dev(y, (z + NZ + SG[d]) % NZ, c, x),
        ).start()

    def r_wait(i, k, d):
        wait_recv(RSR.at[i, d, k - 1, r_rows(k, d), :], rs_r.at[d, k - 1, i])

    def at_chunk(t, lag):
        i = t - lag

        def run(f):
            @pl.when((i >= 0) & (i < NCH))
            def _():
                f(i)

        return run

    def d_ring(p, t, lag, k):
        @at_chunk(t, lag)
        def _(i):
            if k > 1:
                for d in range(2):
                    z_wait(i, k - 1, d)
                    z_send(i, k, d)
                return
            if p == 0:
                zb_in(i).wait()
            if p == 2:
                @pl.when(i >= H)
                def _():
                    wait_recv(XR.at[i], x_r.at[i])

            for d in range(2):
                z_send(i, 1, d, XR.at[i] if p == 2 else None)
            if p == 2:
                ZB[i, zme, :] = XR[i]

    def d_select(p, t, lag):
        @at_chunk(t, lag)
        def _(i):
            for d in range(2):
                z_wait(i, 4, d)
            if p == 2:
                @pl.when(i % H == 0)
                def _():
                    build((x + NX - i // H) % NX, False)
            if p > 0:
                y_sent(i)

            rows = jnp.dot(PM[...], ZB[i], preferred_element_type=F32)
            for n in range(W // 128):
                YS[i, :, n * 128 : (n + 1) * 128] = (rows[:, n * 128 : (n + 1) * 128] * G[...]).astype(BF)
            y_send(i, RV, RB, rv_r)

    def d_consume(p, t, lag):
        @at_chunk(t, lag)
        def _(i):
            y_wait(i, RV, RB, rv_r)
            (consume_grad if p == 2 else consume_inner)(i)

    def y_sent(i):
        wait_send(YS.at[i, pl.ds(0, (NE - 1) * RB), :], y_s.at[i])

    def d_sent():
        @pl.loop(0, NCH)
        def _(i):
            wait_send(ZB.at[i, pl.ds(0, (NZ - 1) * T), :], z_s.at[i])
            y_sent(i)

    def consume_inner(i):
        rows = wide(col(i))

        @pl.loop(0, HID // 256)
        def _(n):
            ln = pl.ds(pl.multiple_of(n * 256, 256), 256)
            IA[:, ln] += jnp.dot(RV[i], DV[rows, ln], preferred_element_type=F32)

    def consume_grad(i):
        xs = (x + NX - i // H) % NX

        @pl.when((i % H == 0) & (i > 0))
        def _():
            wait_recv(AX.at[xs], ax_r.at[xs])

        rows = pl.ds(pl.multiple_of((i % H) * W, W), W)
        IA[rows, :] += lax.dot_general(RV[i], AX[xs], (((0,), (0,)), ((), ())), preferred_element_type=F32)

    def r_final(p, t, lag):
        @at_chunk(t, lag)
        def _(i):
            for d in range(2):
                r_wait(i, 4, d)
            total = PF[i % NPF, zme, :] + RSR[i, 0, 3].astype(F32) + RSR[i, 1, 3].astype(F32)
            term = total.astype(BF)
            if p == 1:
                ZB[i, zme, :] = term
            else:
                lanes_j = wide(col(i))
                grad = (
                    CV[:, lanes_j].astype(F32) + ZB[i, zme, :].astype(F32) + term.astype(F32)
                ).astype(BF)
                ig_ref[:, lanes_j] = grad

                @pl.when(i < H)
                def _():
                    XR[i] = grad

                @pl.when(i >= H)
                def _():
                    XS[i] = grad
                    remote(
                        XS.at[i], XR.at[i], x_s.at[i], x_r.at[i], dev(y, z, c, (x + i // H) % NX)
                    ).start()

    def r_ring(t, lag, k):
        @at_chunk(t, lag)
        def _(i):
            for d in range(2):
                r_wait(i, k - 1, d)
                mine = PF.at[i % NPF, zrow((z + NZ + SG[d] * (5 - k)) % NZ), :]
                if k == 2:
                    half, rest = pl.ds(d * HT, HT), pl.ds((1 - d) * HT, HT)
                    RSS[i, d, 1, rest, :] = mine[rest, :].astype(BF)
                    RSS[i, d, 1, half, :] = (mine[half, :] + RSR[i, d, 0, half, :].astype(F32)).astype(BF)
                else:
                    RSS[i, d, k - 1] = (mine[...] + RSR[i, d, k - 2].astype(F32)).astype(BF)
                r_send(i, k, d)

    def r_combine(t, lag):
        @at_chunk(t, lag)
        def _(i):
            y_wait(i, QV, T, qv_r)
            PF[i % NPF] = jnp.dot(PT[...], QV[i], preferred_element_type=F32)
            for d in range(2):
                far = pl.ds(pl.multiple_of((z + 4) % NZ * T + d * HT, HT), HT)
                RSS[i, d, 0, d * HT : (d + 1) * HT, :] = PF[i % NPF, far, :].astype(BF)
                r_send(i, 1, d)

    def r_piece(t, lag):
        @at_chunk(t, lag)
        def _(i):
            YS[i] = lax.dot_general(
                SC[...], UV[wide(col(i)), :], (((1,), (1,)), ((), ())), preferred_element_type=F32
            ).astype(BF)
            y_send(i, QV, T, qv_r)

    def r_sent():
        @pl.loop(0, NCH)
        def _(i):
            wait_send(ZB.at[i, pl.ds(0, (NZ - 1) * T), :], rs_s.at[i])

    def scale_inner():
        @pl.loop(0, SL // 128)
        def _(n):
            rows = pl.ds(pl.multiple_of(n * 128, 128), 128)
            SC[rows, :] = (IA[rows, :] * SV[rows, :]).astype(BF)
            IA[rows, :] = jnp.zeros((128, HID), F32)

    for copy in ins[:2]:
        copy.wait()
    tabulate()
    ins[2].wait()

    @pl.loop(0, NY)
    def _(b):
        activate(b)

    TGR[x, z] = TV[z]
    pl.semaphore_wait(barrier, NX * NZ - 1 + 3 * NC + 1)

    @pl.loop(0, NCH + 6)
    def _(t):
        for k in (4, 3, 2, 1):
            d_ring(0, t, k - 1, k)

        @pl.when(t == 0)
        def _():
            @pl.loop(1, NX * NZ)
            def _(q):
                xx = (x + q // NZ) % NX
                zz = (z + q) % NZ
                remote(TV.at[zz], TGR.at[x, z], tg_s.at[0], tg_r.at[x], dev(y, zz, c, xx)).start()

        @pl.when(t == 2)
        def _():
            wait_recv(TGR.at[x, pl.ds(0, NZ - 1)], tg_r.at[x])
            build(x, True)

        @pl.when(t == 4)
        def _():
            for dx in range(1, NX):
                xs = (x + dx) % NX
                wait_recv(TGR.at[xs], tg_r.at[xs])
            for copy in ins[3:]:
                copy.wait()
            for dx in range(1, NX):
                remote(AX.at[x], AX.at[x], ax_s.at[0], ax_r.at[x], dev(y, z, c, (x + dx) % NX)).start()

        d_select(0, t, 3)
        d_consume(0, t, 6)

    d_sent()

    for p in (1, 2):
        lag = 4 + p
        scale_inner()

        @pl.loop(0, NCH + 7 + lag)
        def _(t, p=p, lag=lag):
            r_final(p, t, 5)
            d_ring(p, t, lag + 3, 4)
            d_ring(p, t, lag + 2, 3)
            r_ring(t, 4, 4)
            r_piece(t, 0)
            d_consume(p, t, lag + 7)
            d_ring(p, t, lag + 1, 2)
            r_ring(t, 3, 3)
            d_ring(p, t, lag, 1)
            r_ring(t, 2, 2)
            d_select(p, t, lag + 3)
            r_combine(t, 1)

        r_sent()
        d_sent()

    dg_ref[...] = (IA[: H * W, :] * grad_scale).astype(BF)

    @pl.loop(H, NCH)
    def _(i):
        wait_send(XS.at[i], x_s.at[i])

    for _ in range(NX - 1):
        wait_send(AX.at[x], ax_s.at[0])
    wait_send(TGR.at[pl.ds(0, NX - 1)], tg_s.at[0])
    wait_send(TGR.at[x, pl.ds(0, NZ - 1)], tg_s.at[0])


def hand_over(a_ref, b_ref, c_ref, d_ref):
    c_ref[...] = a_ref[...]
    d_ref[...] = b_ref[...]


def body(cotangent, expert_ids, gate_values, hidden_pre, up_weight, down_weight):
    vm, dma = pltpu.VMEM, pltpu.SemaphoreType.DMA
    input_grad, down_grad = pl.pallas_call(
        kernel,
        out_shape=(jax.ShapeDtypeStruct((T, D), BF), jax.ShapeDtypeStruct((H * W, HID), BF)),
        in_specs=[pl.BlockSpec(memory_space=pl.ANY)] * 6,
        out_specs=(pl.BlockSpec(memory_space=pltpu.VMEM),) * 2,
        scratch_shapes=[
            vm((T, D), BF),
            vm(expert_ids.shape[::-1], jnp.int32),
            vm(gate_values.shape[::-1], F32),
            vm((NZ, 2 * NE, T), F32),
            vm((NX, NZ, 2 * NE, T), F32),
            vm((SL, HID), BF),
            vm((SL, HID), F32),
            vm((NX, SL, HID), BF),
            vm((D, HID), BF),
            vm((D, HID), BF),
            vm((SL, ZR), BF),
            vm((ZR, NE * T), BF),
            vm((SL, 128), F32),
            vm((NCH, ZR, W), BF),
            vm((NCH, SL, W), BF),
            vm((NCH, SL, W), BF),
            vm((NCH, NE * T, W), BF),
            vm((SL, HID), F32),
            vm((SL, HID), BF),
            vm((NPF, ZR, W), F32),
            vm((NCH, 2, 4, T, W), BF),
            vm((NCH, 2, 4, T, W), BF),
            vm((NCH, T, W), BF),
            vm((NCH, T, W), BF),
            dma((NCH,)), dma((6,)), dma((1,)), dma((NX,)), dma((1,)), dma((NX,)),
            dma((NCH,)), dma((2, 4, NCH)), dma((NCH,)), dma((NE, NCH)), dma((NE, NCH)),
            dma((NCH,)), dma((2, 4, NCH)), dma((NCH,)), dma((NCH,)),
        ],
        compiler_params=pltpu.CompilerParams(has_side_effects=True, collective_id=0, vmem_limit_bytes=67043328),
        name="layer",
    )(cotangent, expert_ids.T, gate_values.T, hidden_pre[0], up_weight[0], down_weight[0])
    input_grad, down_grad = pl.pallas_call(
        hand_over,
        out_shape=(jax.ShapeDtypeStruct((T, D), BF), jax.ShapeDtypeStruct((H * W, HID), BF)),
        in_specs=[pl.BlockSpec(memory_space=pltpu.VMEM)] * 2,
        out_specs=(pl.BlockSpec(memory_space=pltpu.VMEM),) * 2,
        name="hand_over",
    )(input_grad, down_grad)
    return (input_grad, down_grad[None])


def solution(mesh):
    in_specs = (
        P(("expert", "token"), None),
        P(("expert", "token"), None),
        P(("expert", "token"), None),
        P("expert", "token", None),
        P("expert", None, None),
        P("expert", None, None),
    )
    out_specs = (P(("expert", "token"), None), P("expert", "token", None))
    return jax.shard_map(body, mesh=mesh, in_specs=in_specs, out_specs=out_specs, check_vma=False)
```

```python
import jax
import jax.numpy as jnp
from jax import lax
from jax.experimental import pallas as pl
from jax.experimental.pallas import tpu as pltpu
from jax.sharding import PartitionSpec as P

grad_scale = 0.03125
root_half = 0.7071067811865476
inv_root_two_pi = 0.3989422804014327

NY, NZ, NC, NX = 4, 8, 2, 4
T = 128
D = 2048
HID = 768
CAP = 14
RB = NZ * CAP
NE = NY * NC
SL = NE * RB
H = 2
NCH = NX * H
W = D // NCH
ZR = NZ * T
NPF = 5
BF = jnp.bfloat16
F32 = jnp.float32
MESH = pl.DeviceIdType.MESH


def slope_and_act(hidden_rows):
    values = hidden_rows
    normal_cdf = 0.5 * (1.0 + lax.erf(values * root_half))
    density = inv_root_two_pi * jnp.exp(-0.5 * values * values)
    slopes = normal_cdf + values * density
    active = (values * normal_cdf).astype(jnp.bfloat16)
    return (slopes, active)


def kernel(
    cot_hbm, id_hbm, gate_hbm, hid_hbm, up_hbm, down_hbm,
    ig_ref, dg_ref,
    CV, IDV, GTV, TV, TGR, HV, SV, AX, UV, DV, PM, PT, G, ZB, YS, RV, QV, IA, SC, PF, RSS, RSR, XS, XR,
    l_zb, l_in, tg_s, tg_r, ax_s, ax_r,
    z_s, z_r, y_s, rv_r, qv_r, rs_s, rs_r, x_s, x_r,
):
    ex = lax.axis_index("expert")
    x = lax.axis_index("token")
    y = ex // (NZ * NC)
    z = (ex // NC) % NZ
    c = ex % NC
    me = y * NC + c
    yp, ym, y2 = (y + 1) % NY, (y + NY - 1) % NY, (y + 2) % NY

    def dev(yy, zz, cc, xx):
        return ((yy * NZ + zz) * NC + cc, xx)

    def remote(src, dst, ssem, rsem, target):
        return pltpu.make_async_remote_copy(
            src_ref=src, dst_ref=dst, send_sem=ssem, recv_sem=rsem, device_id=target, device_id_type=MESH
        )

    partner = dev(y, z, 1 - c, x)

    def wait_recv(ref, rsem):
        remote(ref, ref, tg_s.at[0], rsem, partner).wait_recv()

    def wait_send(ref, ssem):
        remote(ref, ref, ssem, tg_r.at[0], partner).wait_send()

    def col(i):
        return (i + x * H) % NCH

    def wide(j):
        return pl.ds(pl.multiple_of(j * W, W), W)

    def zrow(b):
        return pl.ds(pl.multiple_of(b * T, T), T)

    zme = zrow(z)

    barrier = pltpu.get_barrier_semaphore()

    def greet(target):
        pl.semaphore_signal(barrier, inc=1, device_id=target, device_id_type=MESH)

    @pl.loop(1, NX * NZ)
    def _(q):
        greet(dev(y, (z + q) % NZ, c, (x + q // NZ) % NX))

    for cc in range(NC):
        greet(dev(y2, z, cc, x))
        greet(dev(yp, z, cc, x))
        greet(dev(ym, z, cc, x))
    greet(partner)

    def zb_in(i):
        return pltpu.make_async_copy(cot_hbm.at[:, wide(col(i))], ZB.at[i, zme, :], l_zb.at[i])

    ins = [
        pltpu.make_async_copy(id_hbm, IDV, l_in.at[0]),
        pltpu.make_async_copy(gate_hbm, GTV, l_in.at[1]),
        pltpu.make_async_copy(hid_hbm, HV, l_in.at[2]),
        pltpu.make_async_copy(down_hbm, DV, l_in.at[3]),
        pltpu.make_async_copy(up_hbm, UV, l_in.at[4]),
        pltpu.make_async_copy(cot_hbm, CV, l_in.at[5]),
    ]
    for copy in ins[:3]:
        copy.start()

    @pl.loop(0, NCH)
    def _(i):
        zb_in(i).start()

    for copy in ins[3:]:
        copy.start()

    @pl.loop(0, NCH)
    def _(i):
        for o in range(NE):
            QV[i, o * T + RB : (o + 1) * T, :] = jnp.zeros((T - RB, W), BF)

    IA[...] = jnp.zeros_like(IA)

    def tabulate():
        row = lax.broadcasted_iota(jnp.int32, (NZ * NE, T), 0)
        expert = (((row >> 1) & (NY - 1)) * NZ + (row >> 3)) * NC + (row & (NC - 1))
        named, gate = jnp.zeros((NZ * NE, T), F32), jnp.zeros((NZ * NE, T), F32)
        for k in range(IDV.shape[0]):
            hit = IDV[k : k + 1, :] == expert
            named = jnp.where(hit, 1.0, named)
            gate = jnp.where(hit, GTV[k : k + 1, :], gate)
        first = lax.broadcasted_iota(jnp.int32, (T, T), 0)
        second = lax.broadcasted_iota(jnp.int32, (T, T), 1)
        before = jnp.where(first < second, 1.0, 0.0).astype(BF)
        rank = jnp.dot(named.astype(BF), before, preferred_element_type=F32)
        rank = jnp.where(named > 0.0, rank, -1.0)
        for zz in range(NZ):
            TV[zz, :NE, :] = rank[zz * NE : (zz + 1) * NE]
            TV[zz, NE:, :] = gate[zz * NE : (zz + 1) * NE]

    YB = NZ * NC * CAP

    def activate(b):
        new = lax.broadcasted_iota(jnp.int32, (YB, YB), 0).astype(F32)
        core = jnp.where(new >= float(RB), 1.0, 0.0)
        new = new - core * RB
        plane = jnp.floor((new + 0.5) * (1.0 / CAP))
        old = plane * (NC * CAP) + core * CAP + (new - plane * CAP)
        here = lax.broadcasted_iota(jnp.int32, (YB, YB), 1).astype(F32)
        order = jnp.where(here == old, 1.0, 0.0).astype(BF)
        rows = pl.ds(b * YB, YB)
        hidden = jnp.dot(order, HV[rows, :], preferred_element_type=F32)
        slopes, active = slope_and_act(hidden)
        SV[rows, :] = slopes
        AX[x, rows, :] = active

    def build(xs, with_pt):
        @pl.loop(0, NE)
        def _(o):
            gsum = jnp.zeros((RB, 1), F32)
            rows = pl.ds(pl.multiple_of(o * RB, 16), RB)
            for s in range(NZ):
                rank = TGR[xs, s, pl.ds(o, 1), :]
                gate = TGR[xs, s, pl.ds(NE + o, 1), :]
                slot = jnp.where(rank >= 0.0, rank + float(s * CAP), -1.0)
                iota = lax.broadcasted_iota(jnp.int32, (T, T), 0).astype(F32)
                hit = jnp.where(iota == slot, 1.0, 0.0)
                PM[rows, s * T : (s + 1) * T] = hit[:RB].astype(BF)
                gsum = gsum + jnp.sum(hit[:RB] * gate, axis=1, keepdims=True)
                if with_pt:
                    PT[s * T : (s + 1) * T, pl.ds(pl.multiple_of(o * T, T), T)] = hit.T.astype(BF)
            G[rows, :] = jnp.broadcast_to(gsum, (RB, 128))

    def y_send(i, dst, pitch, rsem):
        mine = dst.at[i, pl.ds(pl.multiple_of(me * pitch, 16), RB), :]

        def src(yy, cc):
            return YS.at[i, pl.ds(pl.multiple_of((yy * NC + cc) * RB, 16), RB), :]

        for cc in range(NC):
            remote(src(y2, cc), mine, y_s.at[i], rsem.at[me, i], dev(y2, z, cc, x)).start()
        for cc in range(NC):
            remote(src(yp, cc), mine, y_s.at[i], rsem.at[me, i], dev(yp, z, cc, x)).start()
            remote(src(ym, cc), mine, y_s.at[i], rsem.at[me, i], dev(ym, z, cc, x)).start()
        remote(src(y, 1 - c), mine, y_s.at[i], rsem.at[me, i], partner).start()
        dst[i, pl.ds(pl.multiple_of(me * pitch, 16), RB), :] = YS[
            i, pl.ds(pl.multiple_of(me * RB, 16), RB), :
        ]

    def y_wait(i, dst, pitch, rsem):
        for q in range(1, NE):
            o = (me + q) % NE
            wait_recv(dst.at[i, pl.ds(pl.multiple_of(o * pitch, 16), RB), :], rsem.at[o, i])

    SG = (1, -1)

    HT = T // 2

    def z_ref(i, b, k, d):
        rows = pl.ds(pl.multiple_of(b * T + d * HT, HT), HT) if k == 4 else zrow(b)
        return ZB.at[i, rows, :]

    def z_send(i, k, d, src=None):
        ref = z_ref(i, (z + NZ - SG[d] * (k - 1)) % NZ, k, d)
        remote(
            ref if src is None else src, ref, z_s.at[i], z_r.at[d, k - 1, i], dev(y, (z + NZ + SG[d]) % NZ, c, x)
        ).start()

    def z_wait(i, k, d):
        wait_recv(z_ref(i, (z + NZ - SG[d] * k) % NZ, k, d), z_r.at[d, k - 1, i])

    def r_rows(k, d):
        return pl.ds(d * HT, HT) if k == 1 else pl.ds(0, T)

    def r_send(i, k, d):
        rows = r_rows(k, d)
        remote(
            RSS.at[i, d, k - 1, rows, :],
            RSR.at[i, d, k - 1, rows, :],
            rs_s.at[i],
            rs_r.at[d, k - 1, i],
            dev(y, (z + NZ + SG[d]) % NZ, c, x),
        ).start()

    def r_wait(i, k, d):
        wait_recv(RSR.at[i, d, k - 1, r_rows(k, d), :], rs_r.at[d, k - 1, i])

    def at_chunk(t, lag):
        i = t - lag

        def run(f):
            @pl.when((i >= 0) & (i < NCH))
            def _():
                f(i)

        return run

    def d_ring(p, t, lag, k):
        @at_chunk(t, lag)
        def _(i):
            if k > 1:
                for d in range(2):
                    z_wait(i, k - 1, d)
                    z_send(i, k, d)
                return
            if p == 0:
                zb_in(i).wait()
            if p == 2:
                @pl.when(i >= H)
                def _():
                    wait_recv(XR.at[i], x_r.at[i])

            for d in range(2):
                z_send(i, 1, d, XR.at[i] if p == 2 else None)
            if p == 2:
                ZB[i, zme, :] = XR[i]

    def d_select(p, t, lag):
        @at_chunk(t, lag)
        def _(i):
            for d in range(2):
                z_wait(i, 4, d)
            if p > 0:
                y_sent(i)

            rows = jnp.dot(PM[...], ZB[i], preferred_element_type=F32)
            for n in range(W // 128):
                YS[i, :, n * 128 : (n + 1) * 128] = (rows[:, n * 128 : (n + 1) * 128] * G[...]).astype(BF)
            y_send(i, RV, RB, rv_r)
            if p == 2:
                @pl.when(((i + 1) % H == 0) & (i + 1 < NCH))
                def _():
                    build((x + NX - (i + 1) // H) % NX, False)

    def d_consume(p, t, lag):
        @at_chunk(t, lag)
        def _(i):
            y_wait(i, RV, RB, rv_r)
            (consume_grad if p == 2 else consume_inner)(i)

    def y_sent(i):
        wait_send(YS.at[i, pl.ds(0, (NE - 1) * RB), :], y_s.at[i])

    def d_sent():
        @pl.loop(0, NCH)
        def _(i):
            wait_send(ZB.at[i, pl.ds(0, (NZ - 1) * T), :], z_s.at[i])
            y_sent(i)

    def consume_inner(i):
        rows = wide(col(i))

        @pl.loop(0, HID // 256)
        def _(n):
            ln = pl.ds(pl.multiple_of(n * 256, 256), 256)
            IA[:, ln] += jnp.dot(RV[i], DV[rows, ln], preferred_element_type=F32)

    def consume_grad(i):
        xs = (x + NX - i // H) % NX

        @pl.when((i % H == 0) & (i > 0))
        def _():
            wait_recv(AX.at[xs], ax_r.at[xs])

        rows = pl.ds(pl.multiple_of((i % H) * W, W), W)
        IA[rows, :] += lax.dot_general(RV[i], AX[xs], (((0,), (0,)), ((), ())), preferred_element_type=F32)

    def r_final(p, t, lag):
        @at_chunk(t, lag)
        def _(i):
            for d in range(2):
                r_wait(i, 4, d)
            total = PF[i % NPF, zme, :] + RSR[i, 0, 3].astype(F32) + RSR[i, 1, 3].astype(F32)
            term = total.astype(BF)
            if p == 1:
                ZB[i, zme, :] = term
            else:
                lanes_j = wide(col(i))
                grad = (
                    CV[:, lanes_j].astype(F32) + ZB[i, zme, :].astype(F32) + term.astype(F32)
                ).astype(BF)
                ig_ref[:, lanes_j] = grad

                @pl.when(i < H)
                def _():
                    XR[i] = grad

                @pl.when(i >= H)
                def _():
                    XS[i] = grad
                    remote(
                        XS.at[i], XR.at[i], x_s.at[i], x_r.at[i], dev(y, z, c, (x + i // H) % NX)
                    ).start()

    def r_ring(t, lag, k):
        @at_chunk(t, lag)
        def _(i):
            for d in range(2):
                r_wait(i, k - 1, d)
                mine = PF.at[i % NPF, zrow((z + NZ + SG[d] * (5 - k)) % NZ), :]
                if k == 2:
                    half, rest = pl.ds(d * HT, HT), pl.ds((1 - d) * HT, HT)
                    RSS[i, d, 1, rest, :] = mine[rest, :].astype(BF)
                    RSS[i, d, 1, half, :] = (mine[half, :] + RSR[i, d, 0, half, :].astype(F32)).astype(BF)
                else:
                    RSS[i, d, k - 1] = (mine[...] + RSR[i, d, k - 2].astype(F32)).astype(BF)
                r_send(i, k, d)

    def r_combine(t, lag):
        @at_chunk(t, lag)
        def _(i):
            y_wait(i, QV, T, qv_r)
            PF[i % NPF] = jnp.dot(PT[...], QV[i], preferred_element_type=F32)
            for d in range(2):
                far = pl.ds(pl.multiple_of((z + 4) % NZ * T + d * HT, HT), HT)
                RSS[i, d, 0, d * HT : (d + 1) * HT, :] = PF[i % NPF, far, :].astype(BF)
                r_send(i, 1, d)

    def r_piece(t, lag):
        @at_chunk(t, lag)
        def _(i):
            YS[i] = lax.dot_general(
                SC[...], UV[wide(col(i)), :], (((1,), (1,)), ((), ())), preferred_element_type=F32
            ).astype(BF)
            y_send(i, QV, T, qv_r)

    def r_sent():
        @pl.loop(0, NCH)
        def _(i):
            wait_send(ZB.at[i, pl.ds(0, (NZ - 1) * T), :], rs_s.at[i])

    def scale_inner():
        @pl.loop(0, SL // 128)
        def _(n):
            rows = pl.ds(pl.multiple_of(n * 128, 128), 128)
            SC[rows, :] = (IA[rows, :] * SV[rows, :]).astype(BF)
            IA[rows, :] = jnp.zeros((128, HID), F32)

    for copy in ins[:2]:
        copy.wait()
    tabulate()
    ins[2].wait()

    @pl.loop(0, NY)
    def _(b):
        activate(b)

    TGR[x, z] = TV[z]
    pl.semaphore_wait(barrier, NX * NZ - 1 + 3 * NC + 1)

    @pl.loop(0, NCH + 6)
    def _(t):
        for k in (4, 3, 2, 1):
            d_ring(0, t, k - 1, k)

        @pl.when(t == 0)
        def _():
            @pl.loop(1, NX * NZ)
            def _(q):
                xx = (x + q // NZ) % NX
                zz = (z + q) % NZ
                remote(TV.at[zz], TGR.at[x, z], tg_s.at[0], tg_r.at[x], dev(y, zz, c, xx)).start()

        @pl.when(t == 2)
        def _():
            wait_recv(TGR.at[x, pl.ds(0, NZ - 1)], tg_r.at[x])
            build(x, True)

        @pl.when(t == 4)
        def _():
            for dx in range(1, NX):
                xs = (x + dx) % NX
                wait_recv(TGR.at[xs], tg_r.at[xs])
            for copy in ins[3:]:
                copy.wait()
            for dx in range(1, NX):
                remote(AX.at[x], AX.at[x], ax_s.at[0], ax_r.at[x], dev(y, z, c, (x + dx) % NX)).start()

        d_select(0, t, 3)
        d_consume(0, t, 6)

    d_sent()

    for p in (1, 2):
        lag = 4 + p
        scale_inner()

        @pl.loop(0, NCH + 7 + lag)
        def _(t, p=p, lag=lag):
            r_final(p, t, 5)
            d_ring(p, t, lag + 3, 4)
            d_ring(p, t, lag + 2, 3)
            r_ring(t, 4, 4)
            r_piece(t, 0)
            d_consume(p, t, lag + 7)
            d_ring(p, t, lag + 1, 2)
            r_ring(t, 3, 3)
            d_ring(p, t, lag, 1)
            r_ring(t, 2, 2)
            d_select(p, t, lag + 3)
            r_combine(t, 1)

        r_sent()
        d_sent()

    dg_ref[...] = (IA[: H * W, :] * grad_scale).astype(BF)

    @pl.loop(H, NCH)
    def _(i):
        wait_send(XS.at[i], x_s.at[i])

    for _ in range(NX - 1):
        wait_send(AX.at[x], ax_s.at[0])
    wait_send(TGR.at[pl.ds(0, NX - 1)], tg_s.at[0])
    wait_send(TGR.at[x, pl.ds(0, NZ - 1)], tg_s.at[0])


def hand_over(a_ref, b_ref, c_ref, d_ref):
    c_ref[...] = a_ref[...]
    d_ref[...] = b_ref[...]


def body(cotangent, expert_ids, gate_values, hidden_pre, up_weight, down_weight):
    vm, dma = pltpu.VMEM, pltpu.SemaphoreType.DMA
    input_grad, down_grad = pl.pallas_call(
        kernel,
        out_shape=(jax.ShapeDtypeStruct((T, D), BF), jax.ShapeDtypeStruct((H * W, HID), BF)),
        in_specs=[pl.BlockSpec(memory_space=pl.ANY)] * 6,
        out_specs=(pl.BlockSpec(memory_space=pltpu.VMEM),) * 2,
        scratch_shapes=[
            vm((T, D), BF),
            vm(expert_ids.shape[::-1], jnp.int32),
            vm(gate_values.shape[::-1], F32),
            vm((NZ, 2 * NE, T), F32),
            vm((NX, NZ, 2 * NE, T), F32),
            vm((SL, HID), BF),
            vm((SL, HID), F32),
            vm((NX, SL, HID), BF),
            vm((D, HID), BF),
            vm((D, HID), BF),
            vm((SL, ZR), BF),
            vm((ZR, NE * T), BF),
            vm((SL, 128), F32),
            vm((NCH, ZR, W), BF),
            vm((NCH, SL, W), BF),
            vm((NCH, SL, W), BF),
            vm((NCH, NE * T, W), BF),
            vm((SL, HID), F32),
            vm((SL, HID), BF),
            vm((NPF, ZR, W), F32),
            vm((NCH, 2, 4, T, W), BF),
            vm((NCH, 2, 4, T, W), BF),
            vm((NCH, T, W), BF),
            vm((NCH, T, W), BF),
            dma((NCH,)), dma((6,)), dma((1,)), dma((NX,)), dma((1,)), dma((NX,)),
            dma((NCH,)), dma((2, 4, NCH)), dma((NCH,)), dma((NE, NCH)), dma((NE, NCH)),
            dma((NCH,)), dma((2, 4, NCH)), dma((NCH,)), dma((NCH,)),
        ],
        compiler_params=pltpu.CompilerParams(has_side_effects=True, collective_id=0, vmem_limit_bytes=67043328),
        name="layer",
    )(cotangent, expert_ids.T, gate_values.T, hidden_pre[0], up_weight[0], down_weight[0])
    input_grad, down_grad = pl.pallas_call(
        hand_over,
        out_shape=(jax.ShapeDtypeStruct((T, D), BF), jax.ShapeDtypeStruct((H * W, HID), BF)),
        in_specs=[pl.BlockSpec(memory_space=pltpu.VMEM)] * 2,
        out_specs=(pl.BlockSpec(memory_space=pltpu.VMEM),) * 2,
        name="hand_over",
    )(input_grad, down_grad)
    return (input_grad, down_grad[None])


def solution(mesh):
    in_specs = (
        P(("expert", "token"), None),
        P(("expert", "token"), None),
        P(("expert", "token"), None),
        P("expert", "token", None),
        P("expert", None, None),
        P("expert", None, None),
    )
    out_specs = (P(("expert", "token"), None), P("expert", "token", None))
    return jax.shard_map(body, mesh=mesh, in_specs=in_specs, out_specs=out_specs, check_vma=False)
```
